256 devices in a mesh: dp: 64 (over x, z, core), tensor: 4 (over y).
Axes of the slice: x: 4, y: 4, z: 8, core: 2. Of those that a mesh axis runs over, the one named last changes fastest.
Arguments:
- activations: bfloat16 [768, 8192], P('dp', 'tensor'), may hold values from -400 to 400, as said below
- weight: bfloat16 [8192, 28672], P('dp', 'tensor'), may hold values from -0.0625 to 0.0625
Outputs:
- channel_mean: float32 [8192], P('dp')
- column_errors: float32 [4, 28672], P(None, ('tensor', 'dp'))
- errors: float32 [4], replicated
The draws below stay inside these ranges and needn't reach their ends.
Inputs may be any that keep to these rules, and one draw needn't show every extreme that they name: activations and weight are finite real values within the ranges stated above.
All inputs are finite; a program needn't handle non-finite values.
Results may differ from the reference program's by a relative error of at most 0.0012.
The reference program's roundings to bfloat16 on the way (of `dequant`) count: a program that leaves them out, or rounds other values in their place, can miss the bound.
Values may be sent and summed in bfloat16 or wider, within the bound.
No kernel may reach another device: no remote copies, remote signals or barrier semaphores. Data moves between devices by JAX's collectives and lax.ppermute only.
A program may use at most 128 MiB of HBM per device.

```python
import math
import jax
import jax.numpy as jnp
from jax import lax

D = 8192
F = 28672
GROUP = 128
GRID = 4
TOKENS = 768
N_TENSOR = 4


def draw_activations(key, part):
    base_key = jax.random.fold_in(key, 11)
    key_main, key_row, key_col = jax.random.split(base_key, 3)
    position = jnp.arange(TOKENS, dtype=jnp.float32) / max(TOKENS - 1, 1)
    row_scale = jnp.exp(math.log(4.0) * position + jax.random.uniform(key_row, (TOKENS,), jnp.float32, -0.3, 0.3))
    col_scale = jnp.exp(jax.random.uniform(key_col, (D,), jnp.float32, 0.0, math.log(10.0)))
    values = jnp.clip(jax.random.normal(key_main, (TOKENS, D), jnp.float32), -6.0, 6.0)
    return (values * row_scale[:, None] * col_scale[None, :]).astype(jnp.bfloat16)


def level_of(own_key, shape, cuts, smallest, top_value):
    gain, own = 1.0, jax.random.fold_in(own_key, 6)
    for axis_at, parts in cuts:
        draws = jnp.exp(jax.random.uniform(jax.random.fold_in(own, axis_at), (parts,), jnp.float32, smallest / len(cuts), top_value / len(cuts)))
        gain = gain * jnp.repeat(draws, shape[axis_at] // parts).reshape([-1 if axis == axis_at else 1 for axis in range(len(shape))])
    return gain


def scatter_about(stream_key, extent, spread, limit, cuts=(), kind=jnp.bfloat16):
    entries = spread * jax.random.normal(stream_key, extent, jnp.float32)
    if cuts:
        entries = entries * level_of(stream_key, extent, cuts, -0.22, 0.18)
    return jnp.clip(entries, -limit, limit).astype(kind)


def setup_inputs(seed: int = 0) -> dict:
    splits = jax.random.split(jax.random.key(seed), 3)
    return {
        "activations": draw_activations(jax.random.fold_in(splits[2], 71), 0),
        "weight": scatter_about(splits[1], (D, F), D ** -0.5, 0.0625, ((0, 64), (1, 4))),
    }


def soft_round(values):
    return values - jnp.sin(2.0 * math.pi * values) / (2.0 * math.pi)

def scale_table(channel_mean):
    ratios = jnp.arange(GRID, dtype=jnp.float32) / GRID
    raw = jnp.exp(ratios[:, None] * jnp.log(channel_mean)[None, :])
    top = lax.optimization_barrier(jnp.max(raw, axis=1, keepdims=True))
    bottom = lax.optimization_barrier(jnp.min(raw, axis=1, keepdims=True))
    return raw / jnp.sqrt(top * bottom)

def block_errors(activations, block, scales):
    base_out = jnp.dot(activations, block, preferred_element_type=jnp.float32)
    width = block.shape[1]
    weight_float = block.astype(jnp.float32)

    def one_ratio(factor):
        scaled = weight_float * factor[:, None]
        grouped = scaled.reshape(D // GROUP, GROUP, width)
        quant_step = (lax.optimization_barrier(jnp.max(jnp.abs(grouped), axis=1, keepdims=True)) + 1e-06) / 7.0
        levels = soft_round(grouped / quant_step)
        dequant = ((levels * quant_step).reshape(D, width) / factor[:, None]).astype(jnp.bfloat16)
        quant_out = jnp.dot(activations, dequant, preferred_element_type=jnp.float32)
        residue = quant_out - base_out
        return lax.optimization_barrier(jnp.sum(residue * residue, axis=0))
    return lax.map(one_ratio, scales)

def reference(activations, weight):
    act_float = activations.astype(jnp.float32)
    channel_mean = lax.optimization_barrier(jnp.mean(jnp.abs(act_float), axis=0)) + 1e-06
    scales = scale_table(channel_mean)
    blocks = jnp.transpose(weight.reshape(D, N_TENSOR, F // N_TENSOR), (1, 0, 2))
    column_sums = lax.map(lambda block: block_errors(activations, block, scales), blocks)
    column_sums = jnp.transpose(column_sums, (1, 0, 2)).reshape(GRID, F)
    column_errors = column_sums / TOKENS
    errors = lax.optimization_barrier(jnp.sum(column_sums, axis=1)) / (TOKENS * F)
    return (channel_mean, column_errors, errors)
```

```python
import jax
import jax.numpy as jnp
from jax import lax
from jax.experimental import pallas as pl
from jax.experimental.pallas import tpu as pltpu
from jax.sharding import Mesh
from jax.sharding import PartitionSpec as P

D = 8192
F = 28672
GROUP = 128
GRID = 4
TOKENS = 768
DP = ("dp_0", "dp_1", "dp_2")
ALL = ("dp_0", "dp_1", "dp_2", "tensor")
TENSOR_DP = ("tensor", "dp_0", "dp_1", "dp_2")
ZC = ("dp_1", "dp_2")
YC = ("tensor", "dp_2")
NX, NZ, NC, NY = 4, 8, 2, 4
UNITS = 7
ROWS = 16
UNIT = NX * ROWS
BLOCK = D // NX
GROUPS = BLOCK // GROUP
CHUNKS = (7,)
MIB = 1 << 20

SINE = (
    0.9999996039230294,
    -6.579691569847717,
    12.98643599053418,
    -12.188101430391939,
    6.558041838366218,
    -1.9530314806292366,
)


def vmem(limit):
    return pltpu.CompilerParams(vmem_limit_bytes=limit * MIB)


def starts():
    first, out = 0, []
    for units in CHUNKS:
        out.append(first)
        first += units
    return out


def split_columns(weight_ref, *out_refs):
    for block in range(weight_ref.shape[1] // 128):
        turned = weight_ref[:, block * 128 : (block + 1) * 128].T
        for piece in range(128 // ROWS):
            column = block * 128 + piece * ROWS
            x, rest = divmod(column, F // NY // NX)
            owner, rest = divmod(rest, UNITS * ROWS)
            unit = rest // ROWS
            for out, first, units in zip(out_refs, starts(), CHUNKS):
                if first <= unit < first + units:
                    at = ((unit - first) * NX + x) * ROWS
                    out[owner, at : at + ROWS, :] = turned[piece * ROWS : (piece + 1) * ROWS, :]


def join_tokens(parts_ref, out_ref, sums_ref):
    total = jnp.zeros((1, BLOCK), jnp.float32)
    for part in range(NZ):
        rows = parts_ref[part]
        out_ref[part * 12 : (part + 1) * 12, :] = rows
        total += jnp.sum(jnp.abs(rows.astype(jnp.float32)), axis=0, keepdims=True)
    sums_ref[...] = total


def scale_kernel(sums_ref, mean_ref, scale_ref, inverse_ref):
    mean = jnp.sum(sums_ref[...], axis=1) / TOKENS + 1e-06
    mean_ref[...] = mean
    log = jnp.log(mean)
    for k in range(GRID):
        raw = jnp.exp((k / GRID) * log)
        root = jnp.sqrt(jnp.max(raw) * jnp.min(raw))
        scale = raw / root
        scale_ref[k] = scale
        inverse_ref[k] = 1.0 / scale


def quantize(columns_ref, rows, scale_ref, inverse_ref, delta_ref):
    for group in range(GROUPS):
        packed = columns_ref[group, rows, :]
        wide = packed.astype(jnp.float32)
        for k in range(GRID):
            scaled = wide if k == 0 else wide * scale_ref[k, group : group + 1, :]
            top = jnp.max(jnp.abs(scaled), axis=1, keepdims=True) + 1e-06
            v = scaled * (7.0 / top)
            r = v - jnp.round(v)
            square = r * r
            poly = jnp.full_like(square, SINE[-1])
            for coefficient in SINE[-2::-1]:
                poly = poly * square + coefficient
            shift = (r * poly) * (top * (1.0 / 7.0))
            if k:
                shift = shift * inverse_ref[k, group : group + 1, :]
            dequant = (wide - shift).astype(jnp.bfloat16)
            delta_ref[k * UNIT : (k + 1) * UNIT, group * GROUP : (group + 1) * GROUP] = dequant - packed


def chunk_kernel(units):
    def body(columns_ref, own_ref, other_ref, scale_ref, inverse_ref, out_ref, tokens, delta_0, delta_1):
        half = TOKENS // 2
        tokens[:half, :] = own_ref[...]
        tokens[half:, :] = other_ref[...]
        deltas = (delta_0, delta_1)
        for unit in range(units):
            delta = deltas[unit % 2]
            quantize(columns_ref, pl.ds(unit * UNIT, UNIT), scale_ref, inverse_ref, delta)
            out = lax.dot_general(
                delta[...], tokens[...], (((1,), (1,)), ((), ())), preferred_element_type=jnp.float32
            ).astype(jnp.bfloat16)
            for k in range(GRID):
                for x in range(NX):
                    at = k * UNIT + x * ROWS
                    out_ref[x, unit, k] = out[at : at + ROWS, :]

    return body


def error_kernel(*refs):
    *parts, errors_ref, total_ref = refs
    rows = []
    for k in range(GRID):
        for part in parts:
            for unit in range(part.shape[1]):
                block = part[0, unit, k].astype(jnp.float32)
                for x in range(1, NX):
                    block += part[x, unit, k].astype(jnp.float32)
                block = block * block
                lanes = block[:, :128]
                for at in range(128, TOKENS, 128):
                    lanes += block[:, at : at + 128]
                rows.append(lanes)
    sums = jnp.sum(jnp.concatenate(rows, axis=0).T, axis=0, keepdims=True)
    width = UNITS * ROWS
    for k in range(GRID):
        row = sums[:, k * width : (k + 1) * width]
        errors_ref[k : k + 1, :] = row / TOKENS
        total_ref[:, k : k + 1] = jnp.sum(row, axis=1, keepdims=True)


def spread(value, axes, size):
    wide = jnp.broadcast_to(value[None], (size, *value.shape))
    return lax.all_to_all(wide, axes, 0, 0, tiled=True)


def on_device(activations, weight):
    f32, bf16 = jnp.float32, jnp.bfloat16
    turn = [(x * NY + y, y * NY + x) for x in range(NX) for y in range(NY)]
    turned = lax.ppermute(activations, ("dp_0", "tensor"), turn)
    columns = pl.pallas_call(
        split_columns,
        out_shape=[jax.ShapeDtypeStruct((NZ * NC, u * UNIT, GROUP), bf16) for u in CHUNKS],
        compiler_params=vmem(16),
        name="split_columns",
    )(weight)
    parts = spread(turned, "dp_1", NZ)
    received = [lax.all_to_all(part, ZC, 0, 0, tiled=True) for part in columns]
    joined, sums = pl.pallas_call(
        join_tokens,
        out_shape=[jax.ShapeDtypeStruct((96, BLOCK), bf16), jax.ShapeDtypeStruct((1, BLOCK), f32)],
        compiler_params=vmem(16),
        name="join_tokens",
    )(parts)
    sums = spread(sums, ("dp_0", "tensor", "dp_2"), NX * NY * NC)
    own = spread(joined, "tensor", NY).reshape(TOKENS // 2, BLOCK)
    other = lax.ppermute(own, "dp_2", [(0, 1), (1, 0)])
    mean, scale, inverse = pl.pallas_call(
        scale_kernel,
        out_shape=[
            jax.ShapeDtypeStruct((NX, BLOCK), f32),
            jax.ShapeDtypeStruct((GRID, NX, BLOCK), f32),
            jax.ShapeDtypeStruct((GRID, NX, BLOCK), f32),
        ],
        compiler_params=vmem(16),
        name="scales",
    )(sums.reshape(NX, NY * NC, BLOCK))
    at = lax.axis_index("dp_0")
    mean = lax.dynamic_index_in_dim(mean, at, 0, keepdims=False)
    scale = lax.dynamic_index_in_dim(scale, at, 1, keepdims=False).reshape(GRID, GROUPS, GROUP)
    inverse = lax.dynamic_index_in_dim(inverse, at, 1, keepdims=False).reshape(GRID, GROUPS, GROUP)
    own_mean = lax.dynamic_slice_in_dim(mean, lax.axis_index(ZC) * GROUP, GROUP)

    shares = []
    for units, part in zip(CHUNKS, received):
        partial = pl.pallas_call(
            chunk_kernel(units),
            out_shape=jax.ShapeDtypeStruct((NX, units, GRID, ROWS, TOKENS), bf16),
            scratch_shapes=[
                pltpu.VMEM((TOKENS, BLOCK), bf16),
                pltpu.VMEM((GRID * UNIT, BLOCK), bf16),
                pltpu.VMEM((GRID * UNIT, BLOCK), bf16),
            ],
            compiler_params=vmem(48),
            name="candidates",
        )(part, own, other, scale, inverse)
        shares.append(lax.all_to_all(partial, "dp_0", 0, 0, tiled=True))
    column_errors, totals = pl.pallas_call(
        error_kernel,
        out_shape=[jax.ShapeDtypeStruct((GRID, UNITS * ROWS), f32), jax.ShapeDtypeStruct((1, GRID), f32)],
        compiler_params=vmem(16),
        name="column_errors",
    )(*shares)
    totals = spread(totals, ALL, NX * NY * NZ * NC)
    errors = jnp.sum(totals.reshape(-1, GRID), axis=0) / (TOKENS * F)
    return (own_mean, column_errors, errors)


def solution(mesh):
    torus = Mesh(
        mesh.devices.reshape(NX, NZ, NC, mesh.shape["tensor"]), ("dp_0", "dp_1", "dp_2", "tensor")
    )
    placed = (P(DP, "tensor"), P(DP, "tensor"))
    return jax.shard_map(
        on_device,
        mesh=torus,
        in_specs=placed,
        out_specs=(P(DP), P(None, TENSOR_DP), P()),
        check_vma=False,
    )
```

```python
import jax
import jax.numpy as jnp
from jax import lax
from jax.experimental import pallas as pl
from jax.experimental.pallas import tpu as pltpu
from jax.sharding import Mesh
from jax.sharding import PartitionSpec as P

D = 8192
F = 28672
GROUP = 128
GRID = 4
TOKENS = 768
DP = ("dp_0", "dp_1", "dp_2")
TENSOR_DP = ("tensor", "dp_0", "dp_1", "dp_2")
ZC = ("dp_1", "dp_2")
NX, NZ, NC, NY = 4, 8, 2, 4
UNITS = 7
ROWS = 16
UNIT = NX * ROWS
BLOCK = D // NX
GROUPS = BLOCK // GROUP
SENDS = (3, 4)
PIECES = ((0, 0, 3), (1, 0, 2), (1, 2, 2))
MIB = 1 << 20

SINE = (
    0.9999996039230294,
    -6.579691569847717,
    12.98643599053418,
    -12.188101430391939,
    6.558041838366218,
    -1.9530314806292366,
)


def starts():
    first, out = 0, []
    for units in SENDS:
        out.append(first)
        first += units
    return out


def split_columns(x_ref, weight_ref, *out_refs):
    for block in range(weight_ref.shape[1] // 128):
        turned = weight_ref[:, block * 128 : (block + 1) * 128].T
        for piece in range(128 // ROWS):
            column = block * 128 + piece * ROWS
            x, rest = divmod(column, F // NY // NX)
            owner, rest = divmod(rest, UNITS * ROWS)
            unit = rest // ROWS
            hops = (x + NX - x_ref[0]) % NX
            for out, first, units in zip(out_refs, starts(), SENDS):
                if first <= unit < first + units:
                    at = pl.multiple_of(((unit - first) * NX + hops) * ROWS, ROWS)
                    out[owner, pl.ds(at, ROWS), :] = turned[piece * ROWS : (piece + 1) * ROWS, :]


def join_tokens(parts_ref, out_ref, sums_ref):
    total = jnp.zeros((1, BLOCK), jnp.float32)
    for part in range(NZ):
        rows = parts_ref[part]
        out_ref[part * 12 : (part + 1) * 12, :] = rows
        total += jnp.sum(jnp.abs(rows.astype(jnp.float32)), axis=0, keepdims=True)
    sums_ref[...] = total


def mean_kernel(core_0, core_1, mean_ref):
    mean_ref[...] = (core_0[...] + core_1[...]) / TOKENS + 1e-06


def scale_kernel(mean_0, mean_1, mean_2, mean_3, scale_ref, inverse_ref):
    logs = [jnp.log(mean[...]) for mean in (mean_0, mean_1, mean_2, mean_3)]
    for k in range(GRID):
        raws = [jnp.exp((k / GRID) * log) for log in logs]
        top = jnp.max(jnp.maximum(jnp.maximum(raws[0], raws[1]), jnp.maximum(raws[2], raws[3])))
        bottom = jnp.min(jnp.minimum(jnp.minimum(raws[0], raws[1]), jnp.minimum(raws[2], raws[3])))
        scale = raws[0] / jnp.sqrt(top * bottom)
        scale_ref[k] = scale
        inverse_ref[k] = 1.0 / scale


def quantize(columns_ref, rows, scale_ref, inverse_ref, delta_ref):
    for group in range(GROUPS):
        packed = columns_ref[group, rows, :]
        wide = packed.astype(jnp.float32)
        for k in range(GRID):
            scaled = wide if k == 0 else wide * scale_ref[k, group : group + 1, :]
            top = jnp.max(jnp.abs(scaled), axis=1, keepdims=True) + 1e-06
            v = scaled * (7.0 / top)
            r = v - jnp.round(v)
            square = r * r
            poly = jnp.full_like(square, SINE[-1])
            for coefficient in SINE[-2::-1]:
                poly = poly * square + coefficient
            shift = (r * poly) * (top * (1.0 / 7.0))
            if k:
                shift = shift * inverse_ref[k, group : group + 1, :]
            dequant = (wide - shift).astype(jnp.bfloat16)
            delta_ref[k * UNIT : (k + 1) * UNIT, group * GROUP : (group + 1) * GROUP] = dequant - packed


def piece_kernel(first, units, gathers):
    def body(columns_ref, scale_ref, inverse_ref, *refs):
        if gathers:
            parts, out_refs, tokens, deltas = refs[:8], refs[8:12], refs[12], refs[13:]
            for at, part in enumerate(parts):
                tokens[at * 96 : (at + 1) * 96, :] = part[...]
        else:
            tokens, out_refs, deltas = refs[0], refs[1:5], refs[5:]
        for unit in range(units):
            delta = deltas[unit % 2]
            quantize(columns_ref, pl.ds((first + unit) * UNIT, UNIT), scale_ref, inverse_ref, delta)
            out = lax.dot_general(
                delta[...], tokens[...], (((1,), (1,)), ((), ())), preferred_element_type=jnp.float32
            ).astype(jnp.bfloat16)
            for k in range(GRID):
                for hops in range(NX):
                    at = k * UNIT + hops * ROWS
                    out_refs[hops][unit, k] = out[at : at + ROWS, :]

    return body


def error_kernel(*refs):
    *parts, sums_ref, total_ref = refs
    rows = []
    for k in range(GRID):
        for piece in range(len(PIECES)):
            shares = parts[piece * NX : (piece + 1) * NX]
            for unit in range(shares[0].shape[0]):
                block = shares[0][unit, k].astype(jnp.float32)
                for share in shares[1:]:
                    block += share[unit, k].astype(jnp.float32)
                block = block * block
                lanes = block[:, :128]
                for at in range(128, TOKENS, 128):
                    lanes += block[:, at : at + 128]
                rows.append(lanes)
    sums = jnp.sum(jnp.concatenate(rows, axis=0).T, axis=0, keepdims=True)
    width = UNITS * ROWS
    for k in range(GRID):
        row = sums[:, k * width : (k + 1) * width]
        sums_ref[k : k + 1, :] = row
        total_ref[:, k : k + 1] = jnp.sum(row, axis=1, keepdims=True)


def kernel(body, out_shape, limit=8, flops=0, **more):
    params = pltpu.CompilerParams(vmem_limit_bytes=limit * MIB)
    if flops:
        more["cost_estimate"] = pl.CostEstimate(flops=flops, transcendentals=0, bytes_accessed=0)
    return pl.pallas_call(body, out_shape=out_shape, compiler_params=params, **more)


def spread(value, axes, size):
    wide = jnp.broadcast_to(value[None], (size, *value.shape))
    return lax.all_to_all(wide, axes, 0, 0, tiled=True)


def shifted(value, axis, hops):
    size = lax.axis_size(axis)
    return lax.ppermute(value, axis, [(i, (i + hops) % size) for i in range(size)])


def after(value, *others):
    return lax.optimization_barrier((value, *others))[0]


def search(activations, weight):
    array = jax.ShapeDtypeStruct
    f32, bf16 = jnp.float32, jnp.bfloat16
    turn = [(x * NY + y, y * NY + x) for x in range(NX) for y in range(NY)]
    turned = lax.ppermute(activations, ("dp_0", "tensor"), turn)
    parts = spread(turned, "dp_1", NZ)
    columns = kernel(
        split_columns,
        [array((NZ * NC, u * UNIT, GROUP), bf16) for u in SENDS],
        in_specs=[pl.BlockSpec(memory_space=pltpu.SMEM), pl.BlockSpec(memory_space=pltpu.VMEM)],
    )(lax.axis_index("dp_0").reshape(1), after(weight, turned))
    parts = after(parts, *columns)
    joined, sums = kernel(join_tokens, [array((96, BLOCK), bf16), array((1, BLOCK), f32)])(parts)

    sums = sums.reshape(GROUPS, GROUP)
    around = [shifted(sums, "tensor", hops) for hops in (2, 1, 3)]
    sums = (sums + around[0]) + (around[1] + around[2])
    mean = kernel(mean_kernel, array((GROUPS, GROUP), f32))(sums, shifted(sums, "dp_2", 1))
    around = [shifted(mean, "dp_0", hops) for hops in (2, 1, 3)]
    scale, inverse = kernel(scale_kernel, [array((GRID, GROUPS, GROUP), f32)] * 2)(mean, *around)

    received = []
    for part, gate in zip(columns, ([joined], [scale])):
        part = after(part, *gate, *received)
        received.append(lax.all_to_all(part, ZC, 0, 0, tiled=True))

    tokens = [joined] + [shifted(joined, "tensor", hops) for hops in (2, 1, 3)]
    tokens += [shifted(part, "dp_2", 1) for part in tokens]

    shares = []
    for at, (source, first, units) in enumerate(PIECES):
        gathers = at == 0
        out_shape = [array((units, GRID, ROWS, TOKENS), bf16)] * NX
        if gathers:
            out_shape.append(array((TOKENS, BLOCK), bf16))
        columns = received[source] if gathers else after(received[source], shares[-NX])
        partial = kernel(
            piece_kernel(first, units, gathers),
            out_shape,
            limit=14,
            flops=3 * units * GRID * UNIT * TOKENS * BLOCK,
            scratch_shapes=[pltpu.VMEM((GRID * UNIT, BLOCK), bf16)] * min(units, 2),
        )(columns, scale, inverse, *tokens)
        if gathers:
            tokens = partial[NX:]
        shares += [partial[0]] + [shifted(partial[hops], "dp_0", hops) for hops in (2, 1, 3)]
    sums, totals = kernel(error_kernel, [array((GRID, UNITS * ROWS), f32), array((1, GRID), f32)])(*shares)
    totals = jnp.sum(spread(totals, ("dp_0", "tensor"), NX * NY), axis=0)
    own_mean = lax.dynamic_slice_in_dim(after(mean, sums).reshape(-1), lax.axis_index(ZC) * GROUP, GROUP)
    errors = jnp.sum(spread(totals, ZC, NZ * NC), axis=0).reshape(GRID) / (TOKENS * F)
    column_errors = after(sums, totals) / TOKENS
    return (own_mean, column_errors, errors)


def solution(mesh):
    torus = Mesh(
        mesh.devices.reshape(NX, NZ, NC, mesh.shape["tensor"]), ("dp_0", "dp_1", "dp_2", "tensor")
    )
    placed = (P(DP, "tensor"), P(DP, "tensor"))
    return jax.shard_map(
        search,
        mesh=torus,
        in_specs=placed,
        out_specs=(P(DP), P(None, TENSOR_DP), P()),
        check_vma=False,
    )
```

```python
import jax
import jax.numpy as jnp
from jax import lax
from jax.experimental import pallas as pl
from jax.experimental.pallas import tpu as pltpu
from jax.sharding import Mesh
from jax.sharding import PartitionSpec as P

D = 8192
F = 28672
GROUP = 128
GRID = 4
TOKENS = 768
DP = ("dp_0", "dp_1", "dp_2")
TENSOR_DP = ("tensor", "dp_0", "dp_1", "dp_2")
ZC = ("dp_1", "dp_2")
NX, NZ, NC, NY = 4, 8, 2, 4
UNITS = 7
ROWS = 16
UNIT = NX * ROWS
BLOCK = D // NX
GROUPS = BLOCK // GROUP
SENDS = (4, 3)
PIECES = ((0, 0, 4), (1, 0, 3))
MIB = 1 << 20

SINE = (
    0.9999996039230294,
    -6.579691569847717,
    12.98643599053418,
    -12.188101430391939,
    6.558041838366218,
    -1.9530314806292366,
)


def starts():
    first, out = 0, []
    for units in SENDS:
        out.append(first)
        first += units
    return out


def split_columns(x_ref, weight_ref, *out_refs):
    for block in range(weight_ref.shape[1] // 128):
        turned = weight_ref[:, block * 128 : (block + 1) * 128].T
        for piece in range(128 // ROWS):
            column = block * 128 + piece * ROWS
            x, rest = divmod(column, F // NY // NX)
            owner, rest = divmod(rest, UNITS * ROWS)
            unit = rest // ROWS
            hops = (x + NX - x_ref[0]) % NX
            for out, first, units in zip(out_refs, starts(), SENDS):
                if first <= unit < first + units:
                    at = pl.multiple_of(((unit - first) * NX + hops) * ROWS, ROWS)
                    out[owner, pl.ds(at, ROWS), :] = turned[piece * ROWS : (piece + 1) * ROWS, :]


def pack_tokens(tokens_ref, out_ref):
    out_ref[:12, :] = tokens_ref[:, : BLOCK // 2]
    out_ref[12:, :] = tokens_ref[:, BLOCK // 2 :]


def join_tokens(*refs):
    *parts, out_ref, sums_ref = refs
    for half in range(2):
        total = jnp.zeros((1, BLOCK // 2), jnp.float32)
        lanes = slice(half * BLOCK // 2, (half + 1) * BLOCK // 2)
        for at, part in enumerate(parts):
            rows = part[half * 12 : (half + 1) * 12, :]
            out_ref[at * 12 : (at + 1) * 12, lanes] = rows
            total += jnp.sum(jnp.abs(rows.astype(jnp.float32)), axis=0, keepdims=True)
        sums_ref[:, lanes] = total


def mean_kernel(core_0, core_1, mean_ref):
    mean_ref[...] = (core_0[...] + core_1[...]) / TOKENS + 1e-06


def scale_kernel(mean_0, mean_1, mean_2, mean_3, scale_ref, inverse_ref):
    logs = [jnp.log(mean[...]) for mean in (mean_0, mean_1, mean_2, mean_3)]
    for k in range(GRID):
        raws = [jnp.exp((k / GRID) * log) for log in logs]
        top = jnp.max(jnp.maximum(jnp.maximum(raws[0], raws[1]), jnp.maximum(raws[2], raws[3])))
        bottom = jnp.min(jnp.minimum(jnp.minimum(raws[0], raws[1]), jnp.minimum(raws[2], raws[3])))
        scale = raws[0] / jnp.sqrt(top * bottom)
        scale_ref[k] = scale
        inverse_ref[k] = 1.0 / scale


def quantize(columns_ref, rows, scale_ref, inverse_ref, delta_ref):
    for group in range(GROUPS):
        packed = columns_ref[group, rows, :]
        wide = packed.astype(jnp.float32)
        for k in range(GRID):
            scaled = wide if k == 0 else wide * scale_ref[k, group : group + 1, :]
            top = jnp.max(jnp.abs(scaled), axis=1, keepdims=True) + 1e-06
            v = scaled * (7.0 / top)
            r = v - jnp.round(v)
            square = r * r
            poly = jnp.full_like(square, SINE[-1])
            for coefficient in SINE[-2::-1]:
                poly = poly * square + coefficient
            shift = (r * poly) * (top * (1.0 / 7.0))
            if k:
                shift = shift * inverse_ref[k, group : group + 1, :]
            dequant = (wide - shift).astype(jnp.bfloat16)
            delta_ref[k * UNIT : (k + 1) * UNIT, group * GROUP : (group + 1) * GROUP] = dequant - packed


def piece_kernel(first, units, gathers):
    def body(columns_ref, scale_ref, inverse_ref, *refs):
        if gathers:
            parts, out_refs, tokens, deltas = refs[:8], refs[8:12], refs[12], refs[13:]
            for at, part in enumerate(parts):
                tokens[at * 96 : (at + 1) * 96, :] = part[...]
        else:
            tokens, out_refs, deltas = refs[0], refs[1:5], refs[5:]

        def compute(unit, delta):
            row = (first + unit) * UNIT
            if not isinstance(unit, int):
                row = pl.multiple_of(row, UNIT)
            quantize(columns_ref, pl.ds(row, UNIT), scale_ref, inverse_ref, delta)
            out = lax.dot_general(
                delta[...], tokens[...], (((1,), (1,)), ((), ())), preferred_element_type=jnp.float32
            ).astype(jnp.bfloat16)
            for k in range(GRID):
                for hops in range(NX):
                    at = k * UNIT + hops * ROWS
                    out_refs[hops][unit, k] = out[at : at + ROWS, :]

        def pair(at, carry):
            compute(2 * at, deltas[0])
            compute(2 * at + 1, deltas[1])
            return carry

        if units > 3:
            lax.fori_loop(0, units // 2, pair, 0)
            rest = range(units // 2 * 2, units)
        else:
            rest = range(units)
        for unit in rest:
            compute(unit, deltas[unit % 2])

    return body


def error_kernel(*refs):
    *parts, sums_ref, total_ref = refs
    rows = []
    for k in range(GRID):
        for piece in range(len(PIECES)):
            shares = parts[piece * NX : (piece + 1) * NX]
            for unit in range(shares[0].shape[0]):
                block = shares[0][unit, k].astype(jnp.float32)
                for share in shares[1:]:
                    block += share[unit, k].astype(jnp.float32)
                block = block * block
                lanes = block[:, :128]
                for at in range(128, TOKENS, 128):
                    lanes += block[:, at : at + 128]
                rows.append(lanes)
    sums = jnp.sum(jnp.concatenate(rows, axis=0).T, axis=0, keepdims=True)
    width = UNITS * ROWS
    for k in range(GRID):
        row = sums[:, k * width : (k + 1) * width]
        sums_ref[k : k + 1, :] = row
        total_ref[:, k : k + 1] = jnp.sum(row, axis=1, keepdims=True)


def kernel(body, out_shape, limit=8, flops=0, **more):
    params = pltpu.CompilerParams(vmem_limit_bytes=limit * MIB)
    if flops:
        more["cost_estimate"] = pl.CostEstimate(flops=flops, transcendentals=0, bytes_accessed=0)
    return pl.pallas_call(body, out_shape=out_shape, compiler_params=params, **more)


def spread(value, axes, size):
    wide = jnp.broadcast_to(value[None], (size, *value.shape))
    return lax.all_to_all(wide, axes, 0, 0, tiled=True)


def shifted(value, axis, hops):
    size = lax.axis_size(axis)
    return lax.ppermute(value, axis, [(i, (i + hops) % size) for i in range(size)])


def turned(value, hops):
    where = [(x, z, y) for x in range(NX) for z in range(NZ) for y in range(NY)]
    pairs = [((x * NZ + z) * NY + y, (y * NZ + (z + hops) % NZ) * NY + x) for x, z, y in where]
    return lax.ppermute(value, ("dp_0", "dp_1", "tensor"), pairs)


def after(value, *others):
    return lax.optimization_barrier((value, *others))[0]


def search(activations, weight):
    array = jax.ShapeDtypeStruct
    f32, bf16 = jnp.float32, jnp.bfloat16
    packed = kernel(pack_tokens, array((24, BLOCK // 2), bf16))(activations)
    parts = [turned(packed, hops) for hops in (4, 3, 5, 2, 6, 1, 7, 0)]
    columns = kernel(
        split_columns,
        [array((NZ * NC, u * UNIT, GROUP), bf16) for u in SENDS],
        in_specs=[pl.BlockSpec(memory_space=pltpu.SMEM), pl.BlockSpec(memory_space=pltpu.VMEM)],
    )(lax.axis_index("dp_0").reshape(1), weight)
    joined, sums = kernel(join_tokens, [array((96, BLOCK), bf16), array((1, BLOCK), f32)])(*parts)

    sums = sums.reshape(GROUPS, GROUP)
    around = [shifted(sums, "tensor", hops) for hops in (2, 1, 3)]
    sums = (sums + around[0]) + (around[1] + around[2])
    mean = kernel(mean_kernel, array((GROUPS, GROUP), f32))(sums, shifted(sums, "dp_2", 1))
    around = [shifted(mean, "dp_0", hops) for hops in (2, 1, 3)]
    scale, inverse = kernel(scale_kernel, [array((GRID, GROUPS, GROUP), f32)] * 2)(mean, *around)

    received = []
    for at, part in enumerate(columns):
        if at:
            part = after(part, scale, *received)
        received.append(lax.all_to_all(part, ZC, 0, 0, tiled=True))

    tokens = [joined] + [shifted(joined, "tensor", hops) for hops in (2, 1, 3)]
    tokens += [shifted(part, "dp_2", 1) for part in tokens]

    shares = []
    for at, (source, first, units) in enumerate(PIECES):
        gathers = at == 0
        out_shape = [array((units, GRID, ROWS, TOKENS), bf16)] * NX
        if gathers:
            out_shape.append(array((TOKENS, BLOCK), bf16))
        columns = received[source] if gathers else after(received[source], shares[-NX])
        partial = kernel(
            piece_kernel(first, units, gathers),
            out_shape,
            limit=14,
            flops=3 * units * GRID * UNIT * TOKENS * BLOCK,
            scratch_shapes=[pltpu.VMEM((GRID * UNIT, BLOCK), bf16)] * min(units, 2),
        )(columns, scale, inverse, *tokens)
        if gathers:
            tokens = partial[NX:]
        shares += [partial[0]] + [shifted(partial[hops], "dp_0", hops) for hops in (2, 1, 3)]
    sums, totals = kernel(error_kernel, [array((GRID, UNITS * ROWS), f32), array((1, GRID), f32)])(*shares)
    totals = totals + shifted(totals, "dp_2", 1)
    own_mean = lax.dynamic_slice_in_dim(after(mean, sums).reshape(-1), lax.axis_index(ZC) * GROUP, GROUP)
    errors = jnp.sum(spread(totals, ("dp_0", "dp_1", "tensor"), NX * NZ * NY), axis=0).reshape(GRID) / (TOKENS * F)
    column_errors = after(sums, totals) / TOKENS
    return (own_mean, column_errors, errors)


def solution(mesh):
    torus = Mesh(
        mesh.devices.reshape(NX, NZ, NC, mesh.shape["tensor"]), ("dp_0", "dp_1", "dp_2", "tensor")
    )
    placed = (P(DP, "tensor"), P(DP, "tensor"))
    return jax.shard_map(
        search,
        mesh=torus,
        in_specs=placed,
        out_specs=(P(DP), P(None, TENSOR_DP), P()),
        check_vma=False,
    )
```

```python
import jax
import jax.numpy as jnp
from jax import lax
from jax.experimental import pallas as pl
from jax.experimental.pallas import tpu as pltpu
from jax.sharding import Mesh
from jax.sharding import PartitionSpec as P

D = 8192
F = 28672
GROUP = 128
GRID = 4
TOKENS = 768
DP = ("dp_0", "dp_1", "dp_2")
TENSOR_DP = ("tensor", "dp_0", "dp_1", "dp_2")
ZC = ("dp_1", "dp_2")
NX, NZ, NC, NY = 4, 8, 2, 4
UNITS = 7
ROWS = 16
UNIT = NX * ROWS
BLOCK = D // NX
GROUPS = BLOCK // GROUP
SENDS = (3, 4)
PIECES = ((0, 0, 3), (1, 0, 2), (1, 2, 2))
MIB = 1 << 20

SINE = (
    0.9999996039230294,
    -6.579691569847717,
    12.98643599053418,
    -12.188101430391939,
    6.558041838366218,
    -1.9530314806292366,
)


def starts():
    first, out = 0, []
    for units in SENDS:
        out.append(first)
        first += units
    return out


def split_columns(x_ref, weight_ref, *out_refs):
    for block in range(weight_ref.shape[1] // 128):
        turned = weight_ref[:, block * 128 : (block + 1) * 128].T
        for piece in range(128 // ROWS):
            column = block * 128 + piece * ROWS
            x, rest = divmod(column, F // NY // NX)
            owner, rest = divmod(rest, UNITS * ROWS)
            unit = rest // ROWS
            hops = (x + NX - x_ref[0]) % NX
            for out, first, units in zip(out_refs, starts(), SENDS):
                if first <= unit < first + units:
                    at = pl.multiple_of(((unit - first) * NX + hops) * ROWS, ROWS)
                    out[owner, pl.ds(at, ROWS), :] = turned[piece * ROWS : (piece + 1) * ROWS, :]


def pack_tokens(tokens_ref, out_ref):
    for at in range(NZ):
        out_ref[at, :12, :] = tokens_ref[:, : BLOCK // 2]
        out_ref[at, 12:, :] = tokens_ref[:, BLOCK // 2 :]


def join_tokens(parts_ref, out_ref, sums_ref):
    for half in range(2):
        total = jnp.zeros((1, BLOCK // 2), jnp.float32)
        lanes = slice(half * BLOCK // 2, (half + 1) * BLOCK // 2)
        for at in range(NZ):
            rows = parts_ref[at, half * 12 : (half + 1) * 12, :]
            out_ref[at * 12 : (at + 1) * 12, lanes] = rows
            total += jnp.sum(jnp.abs(rows.astype(jnp.float32)), axis=0, keepdims=True)
        sums_ref[:, lanes] = total


def mean_kernel(core_0, core_1, mean_ref):
    mean_ref[...] = (core_0[...] + core_1[...]) / TOKENS + 1e-06


def scale_kernel(mean_0, mean_1, mean_2, mean_3, scale_ref, inverse_ref):
    logs = [jnp.log(mean[...]) for mean in (mean_0, mean_1, mean_2, mean_3)]
    for k in range(GRID):
        raws = [jnp.exp((k / GRID) * log) for log in logs]
        top = jnp.max(jnp.maximum(jnp.maximum(raws[0], raws[1]), jnp.maximum(raws[2], raws[3])))
        bottom = jnp.min(jnp.minimum(jnp.minimum(raws[0], raws[1]), jnp.minimum(raws[2], raws[3])))
        scale = raws[0] / jnp.sqrt(top * bottom)
        scale_ref[k] = scale
        inverse_ref[k] = 1.0 / scale


def quantize(columns_ref, rows, scale_ref, inverse_ref, delta_ref):
    for group in range(GROUPS):
        packed = columns_ref[group, rows, :]
        wide = packed.astype(jnp.float32)
        for k in range(GRID):
            scaled = wide if k == 0 else wide * scale_ref[k, group : group + 1, :]
            top = jnp.max(jnp.abs(scaled), axis=1, keepdims=True) + 1e-06
            v = scaled * (7.0 / top)
            r = v - jnp.round(v)
            square = r * r
            poly = jnp.full_like(square, SINE[-1])
            for coefficient in SINE[-2::-1]:
                poly = poly * square + coefficient
            shift = (r * poly) * (top * (1.0 / 7.0))
            if k:
                shift = shift * inverse_ref[k, group : group + 1, :]
            dequant = (wide - shift).astype(jnp.bfloat16)
            delta_ref[k * UNIT : (k + 1) * UNIT, group * GROUP : (group + 1) * GROUP] = dequant - packed


def quantize_kernel(columns_ref, scale_ref, inverse_ref, deltas):
    @pl.loop(0, deltas.shape[0])
    def _(unit):
        rows = pl.ds(pl.multiple_of(unit * UNIT, UNIT), UNIT)
        quantize(columns_ref, rows, scale_ref, inverse_ref, deltas.at[unit])


def multiply(delta, tokens, out_refs, unit):
    out = lax.dot_general(
        delta[...], tokens[...], (((1,), (1,)), ((), ())), preferred_element_type=jnp.float32
    ).astype(jnp.bfloat16)
    for k in range(GRID):
        for hops in range(NX):
            at = k * UNIT + hops * ROWS
            out_refs[hops][unit, k] = out[at : at + ROWS, :]


def first_kernel(units):
    def body(*refs):
        deltas, parts, out_refs, tokens = refs[0], refs[1:9], refs[9:13], refs[13]
        for at, part in enumerate(parts):
            tokens[at * 96 : (at + 1) * 96, :] = part[...]
        for unit in range(units):
            multiply(deltas.at[unit], tokens, out_refs, unit)

    return body


def piece_kernel(first, units):
    def body(columns_ref, scale_ref, inverse_ref, tokens, *refs):
        out_refs, deltas = refs[:NX], refs[NX:]
        for unit in range(units):
            delta = deltas[unit % 2]
            rows = slice((first + unit) * UNIT, (first + unit + 1) * UNIT)
            quantize(columns_ref, rows, scale_ref, inverse_ref, delta)
            multiply(delta, tokens, out_refs, unit)

    return body


def error_kernel(*refs):
    *parts, sums_ref, total_ref = refs
    rows = []
    for k in range(GRID):
        for piece in range(len(PIECES)):
            shares = parts[piece * NX : (piece + 1) * NX]
            for unit in range(shares[0].shape[0]):
                block = shares[0][unit, k].astype(jnp.float32)
                for share in shares[1:]:
                    block += share[unit, k].astype(jnp.float32)
                block = block * block
                lanes = block[:, :128]
                for at in range(128, TOKENS, 128):
                    lanes += block[:, at : at + 128]
                rows.append(lanes)
    sums = jnp.sum(jnp.concatenate(rows, axis=0).T, axis=0, keepdims=True)
    width = UNITS * ROWS
    for k in range(GRID):
        row = sums[:, k * width : (k + 1) * width]
        sums_ref[k : k + 1, :] = row
        total_ref[:, k : k + 1] = jnp.sum(row, axis=1, keepdims=True)


def kernel(body, out_shape, limit=14, flops=0, **more):
    params = pltpu.CompilerParams(vmem_limit_bytes=limit * MIB)
    if flops:
        more["cost_estimate"] = pl.CostEstimate(flops=flops, transcendentals=0, bytes_accessed=0)
    return pl.pallas_call(body, out_shape=out_shape, compiler_params=params, **more)


def spread(value, axes, size):
    wide = jnp.broadcast_to(value[None], (size, *value.shape))
    return lax.all_to_all(wide, axes, 0, 0, tiled=True)


def shifted(value, axis, hops):
    size = lax.axis_size(axis)
    return lax.ppermute(value, axis, [(i, (i + hops) % size) for i in range(size)])


def turned(value, hops):
    pairs = [(x * NY + y, y * NY + (x + hops) % NY) for x in range(NX) for y in range(NY)]
    return lax.ppermute(value, ("dp_0", "tensor"), pairs)


def after(value, *others):
    return lax.optimization_barrier((value, *others))[0]


def search(activations, weight):
    array = jax.ShapeDtypeStruct
    f32, bf16 = jnp.float32, jnp.bfloat16
    packed = kernel(pack_tokens, array((NZ, 24, BLOCK // 2), bf16))(activations)
    parts = lax.all_to_all(packed, "dp_1", 0, 0, tiled=True)
    columns = kernel(
        split_columns,
        [array((NZ * NC, u * UNIT, GROUP), bf16) for u in SENDS],
        in_specs=[pl.BlockSpec(memory_space=pltpu.SMEM), pl.BlockSpec(memory_space=pltpu.VMEM)],
    )(lax.axis_index("dp_0").reshape(1), after(weight, packed))
    parts = after(parts, *columns)
    joined, sums = kernel(join_tokens, [array((96, BLOCK), bf16), array((1, BLOCK), f32)])(parts)

    sums = sums.reshape(GROUPS, GROUP)
    around = [turned(sums, hops) for hops in range(NY)]
    sums = (around[0] + around[2]) + (around[1] + around[3])
    mean = kernel(mean_kernel, array((GROUPS, GROUP), f32))(sums, shifted(sums, "dp_2", 1))
    around = [shifted(mean, "dp_0", hops) for hops in (2, 1, 3)]
    scale, inverse = kernel(scale_kernel, [array((GRID, GROUPS, GROUP), f32)] * 2)(mean, *around)

    received = []
    for part, gate in zip(columns, ([joined], [scale])):
        part = after(part, *gate, *received)
        received.append(lax.all_to_all(part, ZC, 0, 0, tiled=True))

    parts = [turned(joined, hops) for hops in range(NY)]
    parts += [shifted(part, "dp_2", 1) for part in parts]

    shares = []
    for at, (source, first, units) in enumerate(PIECES):
        out_shape = [array((units, GRID, ROWS, TOKENS), bf16)] * NX
        work = units * GRID * UNIT * TOKENS * BLOCK
        if at == 0:
            quantized = array((units, GRID * UNIT, BLOCK), bf16)
            deltas = kernel(quantize_kernel, quantized, flops=2 * work)(received[0], scale, inverse)
            *partial, tokens = kernel(
                first_kernel(units), out_shape + [array((TOKENS, BLOCK), bf16)], flops=work
            )(deltas, *parts)
        else:
            partial = kernel(
                piece_kernel(first, units),
                out_shape,
                flops=3 * work,
                scratch_shapes=[pltpu.VMEM((GRID * UNIT, BLOCK), bf16)] * min(units, 2),
            )(after(received[source], shares[-NX]), scale, inverse, tokens)
        shares += [partial[0]] + [shifted(partial[hops], "dp_0", hops) for hops in (2, 1, 3)]
    sums, totals = kernel(error_kernel, [array((GRID, UNITS * ROWS), f32), array((1, GRID), f32)])(*shares)
    own_mean = lax.dynamic_slice_in_dim(after(mean, sums).reshape(-1), lax.axis_index(ZC) * GROUP, GROUP)
    errors = jnp.sum(spread(totals, ("dp_0", "dp_1", "dp_2", "tensor"), NX * NZ * NC * NY), axis=0).reshape(GRID) / (TOKENS * F)
    column_errors = sums / TOKENS
    return (own_mean, column_errors, errors)


def solution(mesh):
    torus = Mesh(
        mesh.devices.reshape(NX, NZ, NC, mesh.shape["tensor"]), ("dp_0", "dp_1", "dp_2", "tensor")
    )
    placed = (P(DP, "tensor"), P(DP, "tensor"))
    return jax.shard_map(
        search,
        mesh=torus,
        in_specs=placed,
        out_specs=(P(DP), P(None, TENSOR_DP), P()),
        check_vma=False,
    )
```

```python
import jax
import jax.numpy as jnp
from jax import lax
from jax.experimental import pallas as pl
from jax.experimental.pallas import tpu as pltpu
from jax.sharding import Mesh
from jax.sharding import PartitionSpec as P

D = 8192
F = 28672
GROUP = 128
GRID = 4
TOKENS = 768
DP = ("dp_0", "dp_1", "dp_2")
TENSOR_DP = ("tensor", "dp_0", "dp_1", "dp_2")
ZC = ("dp_1", "dp_2")
NX, NZ, NC, NY = 4, 8, 2, 4
UNITS = 7
ROWS = 16
UNIT = NX * ROWS
BLOCK = D // NX
GROUPS = BLOCK // GROUP
SENDS = (2, 5)
PIECES = ((0, 0, 2), (1, 0, 3), (1, 3, 2))
MIB = 1 << 20
HALF = BLOCK // 2
OWN = TOKENS // (NX * NZ * NC)
LEAD = OWN * HALF // GROUP

SINE = (
    0.9999996039230294,
    -6.579691569847717,
    12.98643599053418,
    -12.188101430391939,
    6.558041838366218,
    -1.9530314806292366,
)


def starts():
    first, out = 0, []
    for units in SENDS:
        out.append(first)
        first += units
    return out


def split_columns(x_ref, weight_ref, *out_refs):
    for block in range(weight_ref.shape[1] // 128):
        turned = weight_ref[:, block * 128 : (block + 1) * 128].T
        for piece in range(128 // ROWS):
            column = block * 128 + piece * ROWS
            x, rest = divmod(column, F // NY // NX)
            owner, rest = divmod(rest, UNITS * ROWS)
            unit = rest // ROWS
            hops = (x + NX - x_ref[0]) % NX
            for out, first, units in zip(out_refs, starts(), SENDS):
                if first <= unit < first + units:
                    at = pl.multiple_of(((unit - first) * NX + hops) * ROWS, ROWS)
                    out[owner, pl.ds(at, ROWS), :] = turned[piece * ROWS : (piece + 1) * ROWS, :]


def pack_tokens(tokens_ref, out_ref):
    out_ref[:OWN, :] = tokens_ref[:, :HALF]
    out_ref[OWN:, :] = tokens_ref[:, HALF:]


def merge_kernel(tokens_ref, columns_ref, out_ref):
    for half in range(NC):
        for block in range(HALF // GROUP):
            rows = tokens_ref[half * OWN : (half + 1) * OWN, block * GROUP : (block + 1) * GROUP]
            for z in range(NZ):
                out_ref[z * NC + half, block * OWN : (block + 1) * OWN, :] = rows
    out_ref[:, LEAD:, :] = columns_ref[...]


def join_tokens(parts_ref, out_ref, sums_ref):
    for block in range(HALF // GROUP):
        lanes = slice(block * GROUP, (block + 1) * GROUP)
        total = jnp.zeros((OWN, GROUP), jnp.float32)
        for at in range(NZ * NC):
            rows = parts_ref[at, block * OWN : (block + 1) * OWN, :]
            out_ref[at * OWN : (at + 1) * OWN, lanes] = rows
            total += jnp.abs(rows.astype(jnp.float32))
        sums_ref[block : block + 1, :] = jnp.sum(total, axis=0, keepdims=True)


def mean_kernel(core_ref, own_ref, other_ref, mean_ref):
    rows = HALF // GROUP
    own = pl.multiple_of(core_ref[0] * rows, rows)
    other = pl.multiple_of((1 - core_ref[0]) * rows, rows)
    mean_ref[pl.ds(own, rows), :] = own_ref[...] / TOKENS + 1e-06
    mean_ref[pl.ds(other, rows), :] = other_ref[...] / TOKENS + 1e-06


def scale_kernel(mean_0, mean_1, mean_2, mean_3, scale_ref, inverse_ref):
    logs = [jnp.log(mean[...]) for mean in (mean_0, mean_1, mean_2, mean_3)]
    for k in range(GRID):
        raws = [jnp.exp((k / GRID) * log) for log in logs]
        top = jnp.max(jnp.maximum(jnp.maximum(raws[0], raws[1]), jnp.maximum(raws[2], raws[3])))
        bottom = jnp.min(jnp.minimum(jnp.minimum(raws[0], raws[1]), jnp.minimum(raws[2], raws[3])))
        scale = raws[0] / jnp.sqrt(top * bottom)
        scale_ref[k] = scale
        inverse_ref[k] = 1.0 / scale


def quantize(columns_ref, rows, scale_ref, inverse_ref, delta_ref):
    for group in range(GROUPS):
        packed = columns_ref[group, rows, :]
        wide = packed.astype(jnp.float32)
        for k in range(GRID):
            scaled = wide if k == 0 else wide * scale_ref[k, group : group + 1, :]
            top = jnp.max(jnp.abs(scaled), axis=1, keepdims=True) + 1e-06
            v = scaled * (7.0 / top)
            r = v - jnp.round(v)
            square = r * r
            poly = jnp.full_like(square, SINE[-1])
            for coefficient in SINE[-2::-1]:
                poly = poly * square + coefficient
            shift = (r * poly) * (top * (1.0 / 7.0))
            if k:
                shift = shift * inverse_ref[k, group : group + 1, :]
            dequant = (wide - shift).astype(jnp.bfloat16)
            delta_ref[k * UNIT : (k + 1) * UNIT, group * GROUP : (group + 1) * GROUP] = dequant - packed


def quantize_kernel(columns_ref, scale_ref, inverse_ref, deltas):
    @pl.loop(0, deltas.shape[0])
    def _(unit):
        rows = pl.ds(pl.multiple_of(LEAD + unit * UNIT, 32), UNIT)
        quantize(columns_ref, rows, scale_ref, inverse_ref, deltas.at[unit])


def multiply(delta, tokens, out_refs, unit):
    out = lax.dot_general(
        delta[...], tokens[...], (((1,), (1,)), ((), ())), preferred_element_type=jnp.float32
    ).astype(jnp.bfloat16)
    for k in range(GRID):
        for hops in range(NX):
            at = k * UNIT + hops * ROWS
            out_refs[hops][unit, k] = out[at : at + ROWS, :]


def first_kernel(units):
    def body(*refs):
        core_ref, deltas, own, other = refs[0], refs[1], refs[2:6], refs[6:10]
        out_refs, tokens = refs[10:14], refs[14]
        at_own = pl.multiple_of(core_ref[0] * HALF, HALF)
        at_other = pl.multiple_of((1 - core_ref[0]) * HALF, HALF)
        count = TOKENS // NY
        for at in range(NY):
            tokens[at * count : (at + 1) * count, pl.ds(at_own, HALF)] = own[at][...]
            tokens[at * count : (at + 1) * count, pl.ds(at_other, HALF)] = other[at][...]
        for unit in range(units):
            multiply(deltas.at[unit], tokens, out_refs, unit)

    return body


def piece_kernel(first, units):
    def body(columns_ref, scale_ref, inverse_ref, tokens, *refs):
        out_refs, deltas = refs[:NX], refs[NX:]
        for unit in range(units):
            delta = deltas[unit % 2]
            rows = slice((first + unit) * UNIT, (first + unit + 1) * UNIT)
            quantize(columns_ref, rows, scale_ref, inverse_ref, delta)
            multiply(delta, tokens, out_refs, unit)

    return body


def error_kernel(*refs):
    *parts, sums_ref, total_ref = refs
    rows = []
    for k in range(GRID):
        for piece in range(len(PIECES)):
            shares = parts[piece * NX : (piece + 1) * NX]
            for unit in range(shares[0].shape[0]):
                block = shares[0][unit, k].astype(jnp.float32)
                for share in shares[1:]:
                    block += share[unit, k].astype(jnp.float32)
                block = block * block
                lanes = block[:, :128]
                for at in range(128, TOKENS, 128):
                    lanes += block[:, at : at + 128]
                rows.append(lanes)
    sums = jnp.sum(jnp.concatenate(rows, axis=0).T, axis=0, keepdims=True)
    width = UNITS * ROWS
    for k in range(GRID):
        row = sums[:, k * width : (k + 1) * width]
        sums_ref[k : k + 1, :] = row
        total_ref[:, k : k + 1] = jnp.sum(row, axis=1, keepdims=True)


def kernel(body, out_shape, limit=14, flops=0, **more):
    params = pltpu.CompilerParams(vmem_limit_bytes=limit * MIB)
    if flops:
        more["cost_estimate"] = pl.CostEstimate(flops=flops, transcendentals=0, bytes_accessed=0)
    return pl.pallas_call(body, out_shape=out_shape, compiler_params=params, **more)


def spread(value, axes, size):
    wide = jnp.broadcast_to(value[None], (size, *value.shape))
    return lax.all_to_all(wide, axes, 0, 0, tiled=True)


def shifted(value, axis, hops):
    size = lax.axis_size(axis)
    return lax.ppermute(value, axis, [(i, (i + hops) % size) for i in range(size)])


def after(value, *others):
    return lax.optimization_barrier((value, *others))[0]


def search(activations, weight):
    array = jax.ShapeDtypeStruct
    f32, bf16 = jnp.float32, jnp.bfloat16
    smem, local = pl.BlockSpec(memory_space=pltpu.SMEM), pl.BlockSpec(memory_space=pltpu.VMEM)
    core = lax.axis_index("dp_2").reshape(1)
    packed = kernel(pack_tokens, array((NC * OWN, HALF), bf16))(activations)
    turn = [(x * NY + y, y * NY + x) for x in range(NX) for y in range(NY)]
    turned = lax.ppermute(packed, ("dp_0", "tensor"), turn)
    columns = kernel(
        split_columns, [array((NZ * NC, u * UNIT, GROUP), bf16) for u in SENDS], in_specs=[smem, local]
    )(lax.axis_index("dp_0").reshape(1), weight)
    merged = array((NZ * NC, LEAD + SENDS[0] * UNIT, GROUP), bf16)
    merged = kernel(merge_kernel, merged)(turned, columns[0])
    received = [lax.all_to_all(merged, ZC, 0, 0, tiled=True)]
    half = array((HALF // GROUP, GROUP), f32)
    joined, sums = kernel(join_tokens, [array((TOKENS // NY, HALF), bf16), half])(received[0])
    received.append(lax.all_to_all(after(columns[1], joined), ZC, 0, 0, tiled=True))

    around = [shifted(sums, "tensor", hops) for hops in (2, 1, 3)]
    sums = (sums + around[0]) + (around[1] + around[2])
    mean = kernel(
        mean_kernel, array((GROUPS, GROUP), f32), in_specs=[smem, local, local]
    )(core, sums, shifted(sums, "dp_2", 1))
    around = [shifted(mean, "dp_0", hops) for hops in (2, 1, 3)]
    scale, inverse = kernel(scale_kernel, [array((GRID, GROUPS, GROUP), f32)] * 2)(mean, *around)

    parts = [joined] + [shifted(joined, "tensor", hops) for hops in (2, 1, 3)]
    parts += [shifted(part, "dp_2", 1) for part in parts]

    shares = []
    for at, (source, first, units) in enumerate(PIECES):
        out_shape = [array((units, GRID, ROWS, TOKENS), bf16)] * NX
        work = units * GRID * UNIT * TOKENS * BLOCK
        if at == 0:
            quantized = array((units, GRID * UNIT, BLOCK), bf16)
            deltas = kernel(quantize_kernel, quantized, flops=2 * work)(received[0], scale, inverse)
            *partial, tokens = kernel(
                first_kernel(units), out_shape + [array((TOKENS, BLOCK), bf16)], flops=work,
                in_specs=[smem] + [local] * 9,
            )(core, deltas, *parts)
        else:
            partial = kernel(
                piece_kernel(first, units),
                out_shape,
                flops=3 * work,
                scratch_shapes=[pltpu.VMEM((GRID * UNIT, BLOCK), bf16)] * min(units, 2),
            )(after(received[source], shares[-NX]), scale, inverse, tokens)
        shares += [partial[0]] + [shifted(partial[hops], "dp_0", hops) for hops in (2, 1, 3)]
    sums, totals = kernel(error_kernel, [array((GRID, UNITS * ROWS), f32), array((1, GRID), f32)])(*shares)
    own_mean = lax.dynamic_slice_in_dim(after(mean, sums).reshape(-1), lax.axis_index(ZC) * GROUP, GROUP)
    errors = jnp.sum(spread(totals, ("dp_0", "dp_1", "dp_2", "tensor"), NX * NZ * NC * NY), axis=0).reshape(GRID) / (TOKENS * F)
    column_errors = sums / TOKENS
    return (own_mean, column_errors, errors)


def solution(mesh):
    torus = Mesh(
        mesh.devices.reshape(NX, NZ, NC, mesh.shape["tensor"]), ("dp_0", "dp_1", "dp_2", "tensor")
    )
    placed = (P(DP, "tensor"), P(DP, "tensor"))
    return jax.shard_map(
        search,
        mesh=torus,
        in_specs=placed,
        out_specs=(P(DP), P(None, TENSOR_DP), P()),
        check_vma=False,
    )
```

```python
import jax
import jax.numpy as jnp
from jax import lax
from jax.experimental import pallas as pl
from jax.experimental.pallas import tpu as pltpu
from jax.sharding import Mesh
from jax.sharding import PartitionSpec as P

D = 8192
F = 28672
GROUP = 128
GRID = 4
TOKENS = 768
DP = ("dp_0", "dp_1", "dp_2")
TENSOR_DP = ("tensor", "dp_0", "dp_1", "dp_2")
ZC = ("dp_1", "dp_2")
NX, NZ, NC, NY = 4, 8, 2, 4
UNITS = 7
ROWS = 16
UNIT = NX * ROWS
BLOCK = D // NX
GROUPS = BLOCK // GROUP
SENDS = (2, 5)
PIECES = ((0, 0, 2), (1, 0, 3), (1, 3, 2))
MIB = 1 << 20
HALF = BLOCK // 2
OWN = TOKENS // (NX * NZ * NC)
LEAD = OWN * HALF // GROUP

SINE = (
    0.9999996039230294,
    -6.579691569847717,
    12.98643599053418,
    -12.188101430391939,
    6.558041838366218,
    -1.9530314806292366,
)


def starts():
    first, out = 0, []
    for units in SENDS:
        out.append(first)
        first += units
    return out


def split_columns(x_ref, weight_ref, *out_refs):
    for block in range(weight_ref.shape[1] // 128):
        turned = weight_ref[:, block * 128 : (block + 1) * 128].T
        for piece in range(128 // ROWS):
            column = block * 128 + piece * ROWS
            x, rest = divmod(column, F // NY // NX)
            owner, rest = divmod(rest, UNITS * ROWS)
            unit = rest // ROWS
            hops = (x + NX - x_ref[0]) % NX
            for out, first, units in zip(out_refs, starts(), SENDS):
                if first <= unit < first + units:
                    at = pl.multiple_of(((unit - first) * NX + hops) * ROWS, ROWS)
                    out[owner, pl.ds(at, ROWS), :] = turned[piece * ROWS : (piece + 1) * ROWS, :]


def pack_tokens(tokens_ref, out_ref):
    out_ref[:OWN, :] = tokens_ref[:, :HALF]
    out_ref[OWN:, :] = tokens_ref[:, HALF:]


def merge_kernel(tokens_ref, columns_ref, out_ref):
    for half in range(NC):
        for block in range(HALF // GROUP):
            rows = tokens_ref[half * OWN : (half + 1) * OWN, block * GROUP : (block + 1) * GROUP]
            for z in range(NZ):
                out_ref[z * NC + half, block * OWN : (block + 1) * OWN, :] = rows
    out_ref[:, LEAD:, :] = columns_ref[...]


def join_tokens(parts_ref, out_ref, sums_ref):
    for block in range(HALF // GROUP):
        lanes = slice(block * GROUP, (block + 1) * GROUP)
        total = jnp.zeros((OWN, GROUP), jnp.float32)
        for at in range(NZ * NC):
            rows = parts_ref[at, block * OWN : (block + 1) * OWN, :]
            out_ref[at * OWN : (at + 1) * OWN, lanes] = rows
            total += jnp.abs(rows.astype(jnp.float32))
        sums_ref[block : block + 1, :] = jnp.sum(total, axis=0, keepdims=True)


def mean_kernel(core_ref, own_ref, other_ref, mean_ref):
    rows = HALF // GROUP
    own = pl.multiple_of(core_ref[0] * rows, rows)
    other = pl.multiple_of((1 - core_ref[0]) * rows, rows)
    mean_ref[pl.ds(own, rows), :] = own_ref[...] / TOKENS + 1e-06
    mean_ref[pl.ds(other, rows), :] = other_ref[...] / TOKENS + 1e-06


def scale_kernel(mean_0, mean_1, mean_2, mean_3, scale_ref, inverse_ref):
    logs = [jnp.log(mean[...]) for mean in (mean_0, mean_1, mean_2, mean_3)]
    for k in range(GRID):
        raws = [jnp.exp((k / GRID) * log) for log in logs]
        top = jnp.max(jnp.maximum(jnp.maximum(raws[0], raws[1]), jnp.maximum(raws[2], raws[3])))
        bottom = jnp.min(jnp.minimum(jnp.minimum(raws[0], raws[1]), jnp.minimum(raws[2], raws[3])))
        scale = raws[0] / jnp.sqrt(top * bottom)
        scale_ref[k] = scale
        inverse_ref[k] = 1.0 / scale


def quantize(columns_ref, rows, scale_ref, inverse_ref, delta_ref):
    for group in range(GROUPS):
        packed = columns_ref[group, rows, :]
        wide = packed.astype(jnp.float32)
        for k in range(GRID):
            scaled = wide if k == 0 else wide * scale_ref[k, group : group + 1, :]
            top = jnp.max(jnp.abs(scaled), axis=1, keepdims=True) + 1e-06
            v = scaled * (7.0 / top)
            r = v - jnp.round(v)
            square = r * r
            poly = jnp.full_like(square, SINE[-1])
            for coefficient in SINE[-2::-1]:
                poly = poly * square + coefficient
            shift = (r * poly) * (top * (1.0 / 7.0))
            if k:
                shift = shift * inverse_ref[k, group : group + 1, :]
            dequant = (wide - shift).astype(jnp.bfloat16)
            delta_ref[k * UNIT : (k + 1) * UNIT, group * GROUP : (group + 1) * GROUP] = dequant - packed


def quantize_kernel(columns_ref, scale_ref, inverse_ref, deltas):
    @pl.loop(0, deltas.shape[0])
    def _(unit):
        rows = pl.ds(pl.multiple_of(LEAD + unit * UNIT, 32), UNIT)
        quantize(columns_ref, rows, scale_ref, inverse_ref, deltas.at[unit])


def multiply(delta, tokens, out_refs, unit):
    out = lax.dot_general(
        delta[...], tokens[...], (((1,), (1,)), ((), ())), preferred_element_type=jnp.float32
    ).astype(jnp.bfloat16)
    for k in range(GRID):
        for hops in range(NX):
            at = k * UNIT + hops * ROWS
            out_refs[hops][unit, k] = out[at : at + ROWS, :]


def first_kernel(units):
    def body(*refs):
        core_ref, deltas, own, other = refs[0], refs[1], refs[2:6], refs[6:10]
        out_refs, kept, tokens, done = refs[10:14], *refs[14:]
        at_own = pl.multiple_of(core_ref[0] * HALF, HALF)
        at_other = pl.multiple_of((1 - core_ref[0]) * HALF, HALF)
        count = TOKENS // NY
        for at in range(NY):
            tokens[at * count : (at + 1) * count, pl.ds(at_own, HALF)] = own[at][...]
            tokens[at * count : (at + 1) * count, pl.ds(at_other, HALF)] = other[at][...]
        keep = pltpu.make_async_copy(tokens, kept, done)
        keep.start()
        for unit in range(units):
            multiply(deltas.at[unit], tokens, out_refs, unit)
        keep.wait()

    return body


def piece_kernel(first, units):
    def body(columns_ref, scale_ref, inverse_ref, kept, *refs):
        out_refs, (tokens, done), deltas = refs[:NX], refs[NX : NX + 2], refs[NX + 2 :]
        fetch = pltpu.make_async_copy(kept, tokens, done)
        fetch.start()
        for unit in range(units):
            delta = deltas[unit % 2]
            rows = slice((first + unit) * UNIT, (first + unit + 1) * UNIT)
            quantize(columns_ref, rows, scale_ref, inverse_ref, delta)
            if unit == 0:
                fetch.wait()
            multiply(delta, tokens, out_refs, unit)

    return body


def error_kernel(*refs):
    *parts, sums_ref, total_ref = refs
    rows = []
    for k in range(GRID):
        for piece in range(len(PIECES)):
            shares = parts[piece * NX : (piece + 1) * NX]
            for unit in range(shares[0].shape[0]):
                block = shares[0][unit, k].astype(jnp.float32)
                for share in shares[1:]:
                    block += share[unit, k].astype(jnp.float32)
                block = block * block
                lanes = block[:, :128]
                for at in range(128, TOKENS, 128):
                    lanes += block[:, at : at + 128]
                rows.append(lanes)
    sums = jnp.sum(jnp.concatenate(rows, axis=0).T, axis=0, keepdims=True)
    width = UNITS * ROWS
    for k in range(GRID):
        row = sums[:, k * width : (k + 1) * width]
        sums_ref[k : k + 1, :] = row
        total_ref[:, k : k + 1] = jnp.sum(row, axis=1, keepdims=True)


def kernel(body, out_shape, limit=14, flops=0, **more):
    params = pltpu.CompilerParams(vmem_limit_bytes=limit * MIB)
    if flops:
        more["cost_estimate"] = pl.CostEstimate(flops=flops, transcendentals=0, bytes_accessed=0)
    return pl.pallas_call(body, out_shape=out_shape, compiler_params=params, **more)


def spread(value, axes, size):
    wide = jnp.broadcast_to(value[None], (size, *value.shape))
    return lax.all_to_all(wide, axes, 0, 0, tiled=True)


def shifted(value, axis, hops):
    size = lax.axis_size(axis)
    return lax.ppermute(value, axis, [(i, (i + hops) % size) for i in range(size)])


def after(value, *others):
    return lax.optimization_barrier((value, *others))[0]


def search(activations, weight):
    array = jax.ShapeDtypeStruct
    f32, bf16 = jnp.float32, jnp.bfloat16
    smem, local = pl.BlockSpec(memory_space=pltpu.SMEM), pl.BlockSpec(memory_space=pltpu.VMEM)
    core = lax.axis_index("dp_2").reshape(1)
    packed = kernel(pack_tokens, array((NC * OWN, HALF), bf16))(activations)
    turn = [(x * NY + y, y * NY + x) for x in range(NX) for y in range(NY)]
    turned = lax.ppermute(packed, ("dp_0", "tensor"), turn)
    columns = kernel(
        split_columns, [array((NZ * NC, u * UNIT, GROUP), bf16) for u in SENDS], in_specs=[smem, local]
    )(lax.axis_index("dp_0").reshape(1), weight)
    merged = array((NZ * NC, LEAD + SENDS[0] * UNIT, GROUP), bf16)
    merged = kernel(merge_kernel, merged)(turned, columns[0])
    received = [lax.all_to_all(merged, ZC, 0, 0, tiled=True)]
    half = array((HALF // GROUP, GROUP), f32)
    joined, sums = kernel(join_tokens, [array((TOKENS // NY, HALF), bf16), half])(received[0])
    received.append(lax.all_to_all(after(columns[1], joined), ZC, 0, 0, tiled=True))

    around = [shifted(sums, "tensor", hops) for hops in (2, 1, 3)]
    sums = (sums + around[0]) + (around[1] + around[2])
    mean = kernel(
        mean_kernel, array((GROUPS, GROUP), f32), in_specs=[smem, local, local]
    )(core, sums, shifted(sums, "dp_2", 1))
    around = [shifted(mean, "dp_0", hops) for hops in (2, 1, 3)]
    scale, inverse = kernel(scale_kernel, [array((GRID, GROUPS, GROUP), f32)] * 2)(mean, *around)

    parts = [joined] + [shifted(joined, "tensor", hops) for hops in (2, 1, 3)]
    parts += [shifted(part, "dp_2", 1) for part in parts]

    far = pl.BlockSpec(memory_space=pltpu.HBM)
    gathered = [pltpu.VMEM((TOKENS, BLOCK), bf16), pltpu.SemaphoreType.DMA]
    shares = []
    for at, (source, first, units) in enumerate(PIECES):
        out_shape = [array((units, GRID, ROWS, TOKENS), bf16)] * NX
        work = units * GRID * UNIT * TOKENS * BLOCK
        if at == 0:
            quantized = array((units, GRID * UNIT, BLOCK), bf16)
            deltas = kernel(quantize_kernel, quantized, flops=2 * work)(received[0], scale, inverse)
            *partial, tokens = kernel(
                first_kernel(units), out_shape + [pltpu.HBM((TOKENS, BLOCK), bf16)], flops=work,
                in_specs=[smem] + [local] * 9,
                out_specs=[local] * NX + [far],
                scratch_shapes=gathered,
            )(core, deltas, *parts)
        else:
            partial = kernel(
                piece_kernel(first, units),
                out_shape,
                flops=3 * work,
                in_specs=[local] * 3 + [far],
                scratch_shapes=gathered + [pltpu.VMEM((GRID * UNIT, BLOCK), bf16)] * min(units, 2),
            )(after(received[source], shares[-NX]), scale, inverse, pltpu.with_memory_space_constraint(tokens, pltpu.HBM))
        shares += [partial[0]] + [shifted(partial[hops], "dp_0", hops) for hops in (2, 1, 3)]
    sums, totals = kernel(error_kernel, [array((GRID, UNITS * ROWS), f32), array((1, GRID), f32)])(*shares)
    own_mean = lax.dynamic_slice_in_dim(after(mean, sums).reshape(-1), lax.axis_index(ZC) * GROUP, GROUP)
    errors = jnp.sum(spread(totals, ("dp_0", "dp_1", "dp_2", "tensor"), NX * NZ * NC * NY), axis=0).reshape(GRID) / (TOKENS * F)
    column_errors = sums / TOKENS
    return (own_mean, column_errors, errors)


def solution(mesh):
    torus = Mesh(
        mesh.devices.reshape(NX, NZ, NC, mesh.shape["tensor"]), ("dp_0", "dp_1", "dp_2", "tensor")
    )
    placed = (P(DP, "tensor"), P(DP, "tensor"))
    return jax.shard_map(
        search,
        mesh=torus,
        in_specs=placed,
        out_specs=(P(DP), P(None, TENSOR_DP), P()),
        check_vma=False,
    )
```

```python
import jax
import jax.numpy as jnp
from jax import lax
from jax.experimental import pallas as pl
from jax.experimental.pallas import tpu as pltpu
from jax.sharding import Mesh
from jax.sharding import PartitionSpec as P

D = 8192
F = 28672
GROUP = 128
GRID = 4
TOKENS = 768
DP = ("dp_0", "dp_1", "dp_2")
TENSOR_DP = ("tensor", "dp_0", "dp_1", "dp_2")
ZC = ("dp_1", "dp_2")
NX, NZ, NC, NY = 4, 8, 2, 4
UNITS = 7
ROWS = 16
UNIT = NX * ROWS
BLOCK = D // NX
GROUPS = BLOCK // GROUP
SENDS = (1, 2, 4)
PIECES = ((None, 0, 3), (2, 0, 2), (2, 2, 2))
MIB = 1 << 20
HALF = BLOCK // 2
OWN = TOKENS // (NX * NZ * NC)
LEAD = OWN * HALF // GROUP

SINE = (
    0.9999996039230294,
    -6.579691569847717,
    12.98643599053418,
    -12.188101430391939,
    6.558041838366218,
    -1.9530314806292366,
)


def starts():
    first, out = 0, []
    for units in SENDS:
        out.append(first)
        first += units
    return out


def split_columns(x_ref, weight_ref, *out_refs):
    for block in range(weight_ref.shape[1] // 128):
        turned = weight_ref[:, block * 128 : (block + 1) * 128].T
        for piece in range(128 // ROWS):
            column = block * 128 + piece * ROWS
            x, rest = divmod(column, F // NY // NX)
            owner, rest = divmod(rest, UNITS * ROWS)
            unit = rest // ROWS
            hops = (x + NX - x_ref[0]) % NX
            for out, first, units in zip(out_refs, starts(), SENDS):
                if first <= unit < first + units:
                    at = pl.multiple_of(((unit - first) * NX + hops) * ROWS, ROWS)
                    out[owner, pl.ds(at, ROWS), :] = turned[piece * ROWS : (piece + 1) * ROWS, :]


def pack_tokens(tokens_ref, out_ref):
    out_ref[:OWN, :] = tokens_ref[:, :HALF]
    out_ref[OWN:, :] = tokens_ref[:, HALF:]


def merge_kernel(tokens_ref, columns_ref, out_ref):
    for half in range(NC):
        for block in range(HALF // GROUP):
            rows = tokens_ref[half * OWN : (half + 1) * OWN, block * GROUP : (block + 1) * GROUP]
            for z in range(NZ):
                out_ref[z * NC + half, block * OWN : (block + 1) * OWN, :] = rows
    out_ref[:, LEAD:, :] = columns_ref[...]


def join_tokens(parts_ref, out_ref, sums_ref):
    for block in range(HALF // GROUP):
        lanes = slice(block * GROUP, (block + 1) * GROUP)
        total = jnp.zeros((OWN, GROUP), jnp.float32)
        for at in range(NZ * NC):
            rows = parts_ref[at, block * OWN : (block + 1) * OWN, :]
            out_ref[at * OWN : (at + 1) * OWN, lanes] = rows
            total += jnp.abs(rows.astype(jnp.float32))
        sums_ref[block : block + 1, :] = jnp.sum(total, axis=0, keepdims=True)


def mean_kernel(core_ref, own_ref, other_ref, mean_ref):
    rows = HALF // GROUP
    own = pl.multiple_of(core_ref[0] * rows, rows)
    other = pl.multiple_of((1 - core_ref[0]) * rows, rows)
    mean_ref[pl.ds(own, rows), :] = own_ref[...] / TOKENS + 1e-06
    mean_ref[pl.ds(other, rows), :] = other_ref[...] / TOKENS + 1e-06


def scale_kernel(mean_0, mean_1, mean_2, mean_3, scale_ref, inverse_ref):
    logs = [jnp.log(mean[...]) for mean in (mean_0, mean_1, mean_2, mean_3)]
    for k in range(GRID):
        raws = [jnp.exp((k / GRID) * log) for log in logs]
        top = jnp.max(jnp.maximum(jnp.maximum(raws[0], raws[1]), jnp.maximum(raws[2], raws[3])))
        bottom = jnp.min(jnp.minimum(jnp.minimum(raws[0], raws[1]), jnp.minimum(raws[2], raws[3])))
        scale = raws[0] / jnp.sqrt(top * bottom)
        scale_ref[k] = scale
        inverse_ref[k] = 1.0 / scale


def quantize(columns_ref, rows, scale_ref, inverse_ref, delta_ref, group):
    packed = columns_ref[group, rows, :]
    wide = packed.astype(jnp.float32)
    for k in range(GRID):
        scaled = wide if k == 0 else wide * scale_ref[k, pl.ds(group, 1), :]
        top = jnp.max(jnp.abs(scaled), axis=1, keepdims=True) + 1e-06
        v = scaled * (7.0 / top)
        r = v - jnp.round(v)
        square = r * r
        poly = jnp.full_like(square, SINE[-1])
        for coefficient in SINE[-2::-1]:
            poly = poly * square + coefficient
        shift = (r * poly) * (top * (1.0 / 7.0))
        if k:
            shift = shift * inverse_ref[k, pl.ds(group, 1), :]
        dequant = (wide - shift).astype(jnp.bfloat16)
        lanes = group * GROUP if isinstance(group, int) else pl.multiple_of(group * GROUP, GROUP)
        delta_ref[k * UNIT : (k + 1) * UNIT, pl.ds(lanes, GROUP)] = dequant - packed


def quantize_kernel(lead):
    def body(columns_ref, scale_ref, inverse_ref, deltas):
        @pl.loop(0, deltas.shape[0])
        def _(unit):
            rows = pl.ds(pl.multiple_of(lead + unit * UNIT, 32), UNIT)

            @pl.loop(0, GROUPS, step=4)
            def _(group):
                for at in range(4):
                    quantize(columns_ref, rows, scale_ref, inverse_ref, deltas.at[unit], group + at)

    return body


def multiply(delta, tokens, out_refs, unit):
    out = lax.dot_general(
        delta[...], tokens[...], (((1,), (1,)), ((), ())), preferred_element_type=jnp.float32
    ).astype(jnp.bfloat16)
    for k in range(GRID):
        for hops in range(NX):
            at = k * UNIT + hops * ROWS
            out_refs[hops][unit, k] = out[at : at + ROWS, :]


def first_kernel():
    def body(*refs):
        core_ref, deltas, own, other = refs[0], refs[1:3], refs[3:7], refs[7:11]
        out_refs, kept, tokens, done = refs[11:15], *refs[15:]
        at_own = pl.multiple_of(core_ref[0] * HALF, HALF)
        at_other = pl.multiple_of((1 - core_ref[0]) * HALF, HALF)
        count = TOKENS // NY
        for at in range(NY):
            tokens[at * count : (at + 1) * count, pl.ds(at_own, HALF)] = own[at][...]
            tokens[at * count : (at + 1) * count, pl.ds(at_other, HALF)] = other[at][...]
        keep = pltpu.make_async_copy(tokens, kept, done)
        keep.start()
        unit = 0
        for delta in deltas:
            for at in range(delta.shape[0]):
                multiply(delta.at[at], tokens, out_refs, unit)
                unit += 1
        keep.wait()

    return body


def piece_kernel(first, units):
    def body(columns_ref, scale_ref, inverse_ref, kept, *refs):
        out_refs, (tokens, done), deltas = refs[:NX], refs[NX : NX + 2], refs[NX + 2 :]
        fetch = pltpu.make_async_copy(kept, tokens, done)
        fetch.start()
        for unit in range(units):
            delta = deltas[unit % 2]
            rows = slice((first + unit) * UNIT, (first + unit + 1) * UNIT)
            for group in range(GROUPS):
                quantize(columns_ref, rows, scale_ref, inverse_ref, delta, group)
            if unit == 0:
                fetch.wait()
            multiply(delta, tokens, out_refs, unit)

    return body


def error_kernel(*refs):
    *parts, sums_ref, total_ref = refs
    rows = []
    for k in range(GRID):
        for piece in range(len(PIECES)):
            shares = parts[piece * NX : (piece + 1) * NX]
            for unit in range(shares[0].shape[0]):
                block = shares[0][unit, k].astype(jnp.float32)
                for share in shares[1:]:
                    block += share[unit, k].astype(jnp.float32)
                block = block * block
                lanes = block[:, :128]
                for at in range(128, TOKENS, 128):
                    lanes += block[:, at : at + 128]
                rows.append(lanes)
    sums = jnp.sum(jnp.concatenate(rows, axis=0).T, axis=0, keepdims=True)
    width = UNITS * ROWS
    for k in range(GRID):
        row = sums[:, k * width : (k + 1) * width]
        sums_ref[k : k + 1, :] = row
        total_ref[:, k : k + 1] = jnp.sum(row, axis=1, keepdims=True)


def kernel(body, out_shape, limit=14, flops=0, **more):
    params = pltpu.CompilerParams(vmem_limit_bytes=limit * MIB)
    if flops:
        more["cost_estimate"] = pl.CostEstimate(flops=flops, transcendentals=0, bytes_accessed=0)
    return pl.pallas_call(body, out_shape=out_shape, compiler_params=params, **more)


def spread(value, axes, size):
    wide = jnp.broadcast_to(value[None], (size, *value.shape))
    return lax.all_to_all(wide, axes, 0, 0, tiled=True)


def shifted(value, axis, hops):
    size = lax.axis_size(axis)
    return lax.ppermute(value, axis, [(i, (i + hops) % size) for i in range(size)])


def after(value, *others):
    return lax.optimization_barrier((value, *others))[0]


def search(activations, weight):
    array = jax.ShapeDtypeStruct
    f32, bf16 = jnp.float32, jnp.bfloat16
    smem, local = pl.BlockSpec(memory_space=pltpu.SMEM), pl.BlockSpec(memory_space=pltpu.VMEM)
    core = lax.axis_index("dp_2").reshape(1)
    packed = kernel(pack_tokens, array((NC * OWN, HALF), bf16))(activations)
    turn = [(x * NY + y, y * NY + x) for x in range(NX) for y in range(NY)]
    turned = lax.ppermute(packed, ("dp_0", "tensor"), turn)
    columns = kernel(
        split_columns, [array((NZ * NC, u * UNIT, GROUP), bf16) for u in SENDS], in_specs=[smem, local]
    )(lax.axis_index("dp_0").reshape(1), weight)
    merged = array((NZ * NC, LEAD + SENDS[0] * UNIT, GROUP), bf16)
    merged = kernel(merge_kernel, merged)(turned, columns[0])
    received = [lax.all_to_all(merged, ZC, 0, 0, tiled=True)]
    half = array((HALF // GROUP, GROUP), f32)
    joined, sums = kernel(join_tokens, [array((TOKENS // NY, HALF), bf16), half])(received[0])
    for at in (1, 2):
        part = after(columns[at], joined, received[-1])
        received.append(lax.all_to_all(part, ZC, 0, 0, tiled=True))

    around = [shifted(sums, "tensor", hops) for hops in (2, 1, 3)]
    sums = (sums + around[0]) + (around[1] + around[2])
    mean = kernel(
        mean_kernel, array((GROUPS, GROUP), f32), in_specs=[smem, local, local]
    )(core, sums, shifted(sums, "dp_2", 1))
    around = [shifted(mean, "dp_0", hops) for hops in (2, 1, 3)]
    scale, inverse = kernel(scale_kernel, [array((GRID, GROUPS, GROUP), f32)] * 2)(mean, *around)

    parts = [joined] + [shifted(joined, "tensor", hops) for hops in (2, 1, 3)]
    parts += [shifted(part, "dp_2", 1) for part in parts]

    far = pl.BlockSpec(memory_space=pltpu.HBM)
    gathered = [pltpu.VMEM((TOKENS, BLOCK), bf16), pltpu.SemaphoreType.DMA]
    shares = []
    for at, (source, first, units) in enumerate(PIECES):
        out_shape = [array((units, GRID, ROWS, TOKENS), bf16)] * NX
        work = units * GRID * UNIT * TOKENS * BLOCK
        if at == 0:
            deltas = []
            for send, lead in ((0, LEAD), (1, 0)):
                quantized = array((SENDS[send], GRID * UNIT, BLOCK), bf16)
                step = kernel(quantize_kernel(lead), quantized, flops=2 * work)
                deltas.append(step(received[send], scale, inverse))
            *partial, tokens = kernel(
                first_kernel(), out_shape + [pltpu.HBM((TOKENS, BLOCK), bf16)], flops=work,
                in_specs=[smem] + [local] * 10,
                out_specs=[local] * NX + [far],
                scratch_shapes=gathered,
            )(core, *deltas, *parts)
        else:
            partial = kernel(
                piece_kernel(first, units),
                out_shape,
                flops=3 * work,
                in_specs=[local] * 3 + [far],
                scratch_shapes=gathered + [pltpu.VMEM((GRID * UNIT, BLOCK), bf16)] * min(units, 2),
            )(after(received[source], shares[-NX]), scale, inverse, pltpu.with_memory_space_constraint(tokens, pltpu.HBM))
        shares += [partial[0]] + [shifted(partial[hops], "dp_0", hops) for hops in (2, 1, 3)]
    sums, totals = kernel(error_kernel, [array((GRID, UNITS * ROWS), f32), array((1, GRID), f32)])(*shares)
    own_mean = lax.dynamic_slice_in_dim(after(mean, sums).reshape(-1), lax.axis_index(ZC) * GROUP, GROUP)
    errors = jnp.sum(spread(totals, ("dp_0", "dp_1", "dp_2", "tensor"), NX * NZ * NC * NY), axis=0).reshape(GRID) / (TOKENS * F)
    column_errors = sums / TOKENS
    return (own_mean, column_errors, errors)


def solution(mesh):
    torus = Mesh(
        mesh.devices.reshape(NX, NZ, NC, mesh.shape["tensor"]), ("dp_0", "dp_1", "dp_2", "tensor")
    )
    placed = (P(DP, "tensor"), P(DP, "tensor"))
    return jax.shard_map(
        search,
        mesh=torus,
        in_specs=placed,
        out_specs=(P(DP), P(None, TENSOR_DP), P()),
        check_vma=False,
    )
```

```python
import jax
import jax.numpy as jnp
from jax import lax
from jax.experimental import pallas as pl
from jax.experimental.pallas import tpu as pltpu
from jax.sharding import Mesh
from jax.sharding import PartitionSpec as P

D = 8192
F = 28672
GROUP = 128
GRID = 4
TOKENS = 768
DP = ("dp_0", "dp_1", "dp_2")
TENSOR_DP = ("tensor", "dp_0", "dp_1", "dp_2")
ZC = ("dp_1", "dp_2")
NX, NZ, NC, NY = 4, 8, 2, 4
UNITS = 7
ROWS = 16
UNIT = NX * ROWS
BLOCK = D // NX
GROUPS = BLOCK // GROUP
SENDS = (1, 3, 3)
PIECES = ((None, 0, 4), (2, 0, 3))
MIB = 1 << 20
HALF = BLOCK // 2
OWN = TOKENS // (NX * NZ * NC)
LEAD = OWN * HALF // GROUP

SINE = tuple(
    c / 7.0
    for c in (
        0.9999996039230294,
        -6.579691569847717,
        12.98643599053418,
        -12.188101430391939,
        6.558041838366218,
        -1.9530314806292366,
    )
)


def starts():
    first, out = 0, []
    for units in SENDS:
        out.append(first)
        first += units
    return out


def split_columns(x_ref, weight_ref, *out_refs):
    for block in range(weight_ref.shape[1] // 128):
        turned = weight_ref[:, block * 128 : (block + 1) * 128].T
        for piece in range(128 // ROWS):
            column = block * 128 + piece * ROWS
            x, rest = divmod(column, F // NY // NX)
            owner, rest = divmod(rest, UNITS * ROWS)
            unit = rest // ROWS
            hops = (x + NX - x_ref[0]) % NX
            for out, first, units in zip(out_refs, starts(), SENDS):
                if first <= unit < first + units:
                    at = pl.multiple_of(((unit - first) * NX + hops) * ROWS, ROWS)
                    out[owner, pl.ds(at, ROWS), :] = turned[piece * ROWS : (piece + 1) * ROWS, :]


def pack_tokens(tokens_ref, out_ref):
    out_ref[:OWN, :] = tokens_ref[:, :HALF]
    out_ref[OWN:, :] = tokens_ref[:, HALF:]


def merge_kernel(tokens_ref, columns_ref, out_ref):
    for half in range(NC):
        for block in range(HALF // GROUP):
            rows = tokens_ref[half * OWN : (half + 1) * OWN, block * GROUP : (block + 1) * GROUP]
            for z in range(NZ):
                out_ref[z * NC + half, block * OWN : (block + 1) * OWN, :] = rows
    out_ref[:, LEAD:, :] = columns_ref[...]


def join_tokens(parts_ref, out_ref, sums_ref):
    for block in range(HALF // GROUP):
        lanes = slice(block * GROUP, (block + 1) * GROUP)
        total = jnp.zeros((OWN, GROUP), jnp.float32)
        for at in range(NZ * NC):
            rows = parts_ref[at, block * OWN : (block + 1) * OWN, :]
            out_ref[at * OWN : (at + 1) * OWN, lanes] = rows
            total += jnp.abs(rows.astype(jnp.float32))
        sums_ref[block : block + 1, :] = jnp.sum(total, axis=0, keepdims=True)


def mean_kernel(core_ref, own_ref, other_ref, mean_ref):
    rows = HALF // GROUP
    own = pl.multiple_of(core_ref[0] * rows, rows)
    other = pl.multiple_of((1 - core_ref[0]) * rows, rows)
    mean_ref[pl.ds(own, rows), :] = own_ref[...] / TOKENS + 1e-06
    mean_ref[pl.ds(other, rows), :] = other_ref[...] / TOKENS + 1e-06


def scale_kernel(mean_0, mean_1, mean_2, mean_3, scale_ref, inverse_ref):
    logs = [jnp.log(mean[...]) for mean in (mean_0, mean_1, mean_2, mean_3)]
    for k in range(GRID):
        raws = [jnp.exp((k / GRID) * log) for log in logs]
        top = jnp.max(jnp.maximum(jnp.maximum(raws[0], raws[1]), jnp.maximum(raws[2], raws[3])))
        bottom = jnp.min(jnp.minimum(jnp.minimum(raws[0], raws[1]), jnp.minimum(raws[2], raws[3])))
        scale = raws[0] / jnp.sqrt(top * bottom)
        scale_ref[k] = scale
        inverse_ref[k] = 1.0 / scale


def quantize(columns_ref, rows, scale_ref, inverse_ref, delta_ref, group):
    packed = columns_ref[group, rows, :]
    wide = packed.astype(jnp.float32)
    for k in range(GRID):
        scaled = wide if k == 0 else wide * scale_ref[k, pl.ds(group, 1), :]
        top = jnp.max(jnp.abs(scaled), axis=1, keepdims=True) + 1e-06
        v = scaled * (7.0 / top)
        r = v - jnp.round(v)
        square = r * r
        poly = jnp.full_like(square, SINE[-1])
        for coefficient in SINE[-2::-1]:
            poly = poly * square + coefficient
        shift = (r * poly) * top
        if k:
            shift = shift * inverse_ref[k, pl.ds(group, 1), :]
        dequant = (wide - shift).astype(jnp.bfloat16)
        lanes = group * GROUP if isinstance(group, int) else pl.multiple_of(group * GROUP, GROUP)
        delta_ref[k * UNIT : (k + 1) * UNIT, pl.ds(lanes, GROUP)] = dequant - packed


def quantize_kernel(lead):
    def body(columns_ref, scale_ref, inverse_ref, deltas):
        @pl.loop(0, deltas.shape[0])
        def _(unit):
            rows = pl.ds(pl.multiple_of(lead + unit * UNIT, 32), UNIT)

            @pl.loop(0, GROUPS, step=4)
            def _(group):
                for at in range(4):
                    quantize(columns_ref, rows, scale_ref, inverse_ref, deltas.at[unit], group + at)

    return body


def multiply(delta, tokens, out_refs, unit):
    out = lax.dot_general(
        delta[...], tokens[...], (((1,), (1,)), ((), ())), preferred_element_type=jnp.float32
    ).astype(jnp.bfloat16)
    for k in range(GRID):
        for hops in range(NX):
            at = k * UNIT + hops * ROWS
            out_refs[hops][unit, k] = out[at : at + ROWS, :]


def first_kernel():
    def body(*refs):
        core_ref, deltas, own, other = refs[0], refs[1:3], refs[3:7], refs[7:11]
        out_refs, kept, tokens, done = refs[11:15], *refs[15:]
        at_own = pl.multiple_of(core_ref[0] * HALF, HALF)
        at_other = pl.multiple_of((1 - core_ref[0]) * HALF, HALF)
        count = TOKENS // NY
        for at in range(NY):
            tokens[at * count : (at + 1) * count, pl.ds(at_own, HALF)] = own[at][...]
            tokens[at * count : (at + 1) * count, pl.ds(at_other, HALF)] = other[at][...]
        keep = pltpu.make_async_copy(tokens, kept, done)
        keep.start()
        unit = 0
        for delta in deltas:
            for at in range(delta.shape[0]):
                multiply(delta.at[at], tokens, out_refs, unit)
                unit += 1
        keep.wait()

    return body


def piece_kernel(first, units):
    def body(columns_ref, scale_ref, inverse_ref, kept, *refs):
        out_refs, (tokens, done), deltas = refs[:NX], refs[NX : NX + 2], refs[NX + 2 :]
        fetch = pltpu.make_async_copy(kept, tokens, done)
        fetch.start()
        for unit in range(units):
            delta = deltas[unit % 2]
            rows = slice((first + unit) * UNIT, (first + unit + 1) * UNIT)
            for group in range(GROUPS):
                quantize(columns_ref, rows, scale_ref, inverse_ref, delta, group)
            if unit == 0:
                fetch.wait()
            multiply(delta, tokens, out_refs, unit)

    return body


def error_kernel(*refs):
    *parts, sums_ref, total_ref = refs
    rows = []
    for k in range(GRID):
        for piece in range(len(PIECES)):
            shares = parts[piece * NX : (piece + 1) * NX]
            for unit in range(shares[0].shape[0]):
                block = shares[0][unit, k].astype(jnp.float32)
                for share in shares[1:]:
                    block += share[unit, k].astype(jnp.float32)
                block = block * block
                lanes = block[:, :128]
                for at in range(128, TOKENS, 128):
                    lanes += block[:, at : at + 128]
                rows.append(lanes)
    sums = jnp.sum(jnp.concatenate(rows, axis=0).T, axis=0, keepdims=True)
    width = UNITS * ROWS
    for k in range(GRID):
        row = sums[:, k * width : (k + 1) * width]
        sums_ref[k : k + 1, :] = row
        total_ref[:, k : k + 1] = jnp.sum(row, axis=1, keepdims=True)


def kernel(body, out_shape, limit=14, flops=0, **more):
    params = pltpu.CompilerParams(vmem_limit_bytes=limit * MIB)
    if flops:
        more["cost_estimate"] = pl.CostEstimate(flops=flops, transcendentals=0, bytes_accessed=0)
    return pl.pallas_call(body, out_shape=out_shape, compiler_params=params, **more)


def spread(value, axes, size):
    wide = jnp.broadcast_to(value[None], (size, *value.shape))
    return lax.all_to_all(wide, axes, 0, 0, tiled=True)


def shifted(value, axis, hops):
    size = lax.axis_size(axis)
    return lax.ppermute(value, axis, [(i, (i + hops) % size) for i in range(size)])


def after(value, *others):
    return lax.optimization_barrier((value, *others))[0]


def search(activations, weight):
    array = jax.ShapeDtypeStruct
    f32, bf16 = jnp.float32, jnp.bfloat16
    smem, local = pl.BlockSpec(memory_space=pltpu.SMEM), pl.BlockSpec(memory_space=pltpu.VMEM)
    core = lax.axis_index("dp_2").reshape(1)
    packed = kernel(pack_tokens, array((NC * OWN, HALF), bf16))(activations)
    turn = [(x * NY + y, y * NY + x) for x in range(NX) for y in range(NY)]
    turned = lax.ppermute(packed, ("dp_0", "tensor"), turn)
    columns = kernel(
        split_columns, [array((NZ * NC, u * UNIT, GROUP), bf16) for u in SENDS], in_specs=[smem, local]
    )(lax.axis_index("dp_0").reshape(1), weight)
    merged = array((NZ * NC, LEAD + SENDS[0] * UNIT, GROUP), bf16)
    merged = kernel(merge_kernel, merged)(turned, columns[0])
    received = [lax.all_to_all(merged, ZC, 0, 0, tiled=True)]
    half = array((HALF // GROUP, GROUP), f32)
    joined, sums = kernel(join_tokens, [array((TOKENS // NY, HALF), bf16), half])(received[0])
    for at in (1, 2):
        part = after(columns[at], joined, received[-1])
        received.append(lax.all_to_all(part, ZC, 0, 0, tiled=True))

    around = [shifted(sums, "tensor", hops) for hops in (2, 1, 3)]
    sums = (sums + around[0]) + (around[1] + around[2])
    mean = kernel(
        mean_kernel, array((GROUPS, GROUP), f32), in_specs=[smem, local, local]
    )(core, sums, shifted(sums, "dp_2", 1))
    around = [shifted(mean, "dp_0", hops) for hops in (2, 1, 3)]
    scale, inverse = kernel(scale_kernel, [array((GRID, GROUPS, GROUP), f32)] * 2)(mean, *around)

    parts = [joined] + [shifted(joined, "tensor", hops) for hops in (2, 1, 3)]
    parts += [shifted(part, "dp_2", 1) for part in parts]

    far = pl.BlockSpec(memory_space=pltpu.HBM)
    gathered = [pltpu.VMEM((TOKENS, BLOCK), bf16), pltpu.SemaphoreType.DMA]
    shares = []
    for at, (source, first, units) in enumerate(PIECES):
        out_shape = [array((units, GRID, ROWS, TOKENS), bf16)] * NX
        work = units * GRID * UNIT * TOKENS * BLOCK
        if at == 0:
            deltas = []
            for send, lead in ((0, LEAD), (1, 0)):
                quantized = array((SENDS[send], GRID * UNIT, BLOCK), bf16)
                step = kernel(quantize_kernel(lead), quantized, flops=2 * work)
                deltas.append(step(received[send], scale, inverse))
            *partial, tokens = kernel(
                first_kernel(), out_shape + [pltpu.HBM((TOKENS, BLOCK), bf16)], flops=work,
                in_specs=[smem] + [local] * 10,
                out_specs=[local] * NX + [far],
                scratch_shapes=gathered,
            )(core, *deltas, *parts)
        else:
            partial = kernel(
                piece_kernel(first, units),
                out_shape,
                flops=3 * work,
                in_specs=[local] * 3 + [far],
                scratch_shapes=gathered + [pltpu.VMEM((GRID * UNIT, BLOCK), bf16)] * min(units, 2),
            )(after(received[source], shares[-NX]), scale, inverse, pltpu.with_memory_space_constraint(tokens, pltpu.HBM))
        shares += [partial[0]] + [shifted(partial[hops], "dp_0", hops) for hops in (2, 1, 3)]
    sums, totals = kernel(error_kernel, [array((GRID, UNITS * ROWS), f32), array((1, GRID), f32)])(*shares)
    own_mean = lax.dynamic_slice_in_dim(after(mean, sums).reshape(-1), lax.axis_index(ZC) * GROUP, GROUP)
    errors = jnp.sum(spread(totals, ("dp_0", "dp_1", "dp_2", "tensor"), NX * NZ * NC * NY), axis=0).reshape(GRID) / (TOKENS * F)
    column_errors = sums / TOKENS
    return (own_mean, column_errors, errors)


def solution(mesh):
    torus = Mesh(
        mesh.devices.reshape(NX, NZ, NC, mesh.shape["tensor"]), ("dp_0", "dp_1", "dp_2", "tensor")
    )
    placed = (P(DP, "tensor"), P(DP, "tensor"))
    return jax.shard_map(
        search,
        mesh=torus,
        in_specs=placed,
        out_specs=(P(DP), P(None, TENSOR_DP), P()),
        check_vma=False,
    )
```

```python
import jax
import jax.numpy as jnp
from jax import lax
from jax.experimental import pallas as pl
from jax.experimental.pallas import tpu as pltpu
from jax.sharding import Mesh
from jax.sharding import PartitionSpec as P

D = 8192
F = 28672
GROUP = 128
GRID = 4
TOKENS = 768
DP = ("dp_0", "dp_1", "dp_2")
TENSOR_DP = ("tensor", "dp_0", "dp_1", "dp_2")
ZC = ("dp_1", "dp_2")
NX, NZ, NC, NY = 4, 8, 2, 4
UNITS = 7
ROWS = 16
UNIT = NX * ROWS
BLOCK = D // NX
GROUPS = BLOCK // GROUP
SENDS = (1, 2, 4)
PIECES = ((None, 0, 3), (2, 0, 2), (2, 2, 2))
MIB = 1 << 20
HALF = BLOCK // 2
OWN = TOKENS // (NX * NZ * NC)
LEAD = OWN * HALF // GROUP

SINE = tuple(
    c / 7.0
    for c in (
        0.9999996039230294,
        -6.579691569847717,
        12.98643599053418,
        -12.188101430391939,
        6.558041838366218,
        -1.9530314806292366,
    )
)


def starts():
    first, out = 0, []
    for units in SENDS:
        out.append(first)
        first += units
    return out


def split_columns(x_ref, weight_ref, *out_refs):
    for block in range(weight_ref.shape[1] // 128):
        turned = weight_ref[:, block * 128 : (block + 1) * 128].T
        for piece in range(128 // ROWS):
            column = block * 128 + piece * ROWS
            x, rest = divmod(column, F // NY // NX)
            owner, rest = divmod(rest, UNITS * ROWS)
            unit = rest // ROWS
            hops = (x + NX - x_ref[0]) % NX
            for out, first, units in zip(out_refs, starts(), SENDS):
                if first <= unit < first + units:
                    at = pl.multiple_of(((unit - first) * NX + hops) * ROWS, ROWS)
                    out[owner, pl.ds(at, ROWS), :] = turned[piece * ROWS : (piece + 1) * ROWS, :]


def pack_tokens(tokens_ref, out_ref):
    out_ref[:OWN, :] = tokens_ref[:, :HALF]
    out_ref[OWN:, :] = tokens_ref[:, HALF:]


def merge_kernel(tokens_ref, columns_ref, out_ref):
    for half in range(NC):
        for block in range(HALF // GROUP):
            rows = tokens_ref[half * OWN : (half + 1) * OWN, block * GROUP : (block + 1) * GROUP]
            for z in range(NZ):
                out_ref[z * NC + half, block * OWN : (block + 1) * OWN, :] = rows
    out_ref[:, LEAD:, :] = columns_ref[...]


def join_tokens(parts_ref, out_ref, sums_ref):
    for block in range(HALF // GROUP):
        lanes = slice(block * GROUP, (block + 1) * GROUP)
        total = jnp.zeros((OWN, GROUP), jnp.float32)
        for at in range(NZ * NC):
            rows = parts_ref[at, block * OWN : (block + 1) * OWN, :]
            out_ref[at * OWN : (at + 1) * OWN, lanes] = rows
            total += jnp.abs(rows.astype(jnp.float32))
        sums_ref[block : block + 1, :] = jnp.sum(total, axis=0, keepdims=True)


def mean_kernel(core_ref, own_ref, other_ref, mean_ref):
    rows = HALF // GROUP
    own = pl.multiple_of(core_ref[0] * rows, rows)
    other = pl.multiple_of((1 - core_ref[0]) * rows, rows)
    mean_ref[pl.ds(own, rows), :] = own_ref[...] / TOKENS + 1e-06
    mean_ref[pl.ds(other, rows), :] = other_ref[...] / TOKENS + 1e-06


def scale_kernel(mean_0, mean_1, mean_2, mean_3, scale_ref, inverse_ref):
    logs = [jnp.log(mean[...]) for mean in (mean_0, mean_1, mean_2, mean_3)]
    for k in range(GRID):
        raws = [jnp.exp((k / GRID) * log) for log in logs]
        top = jnp.max(jnp.maximum(jnp.maximum(raws[0], raws[1]), jnp.maximum(raws[2], raws[3])))
        bottom = jnp.min(jnp.minimum(jnp.minimum(raws[0], raws[1]), jnp.minimum(raws[2], raws[3])))
        scale = raws[0] / jnp.sqrt(top * bottom)
        scale_ref[k] = scale
        inverse_ref[k] = 1.0 / scale


def quantize(columns_ref, rows, scale_ref, inverse_ref, delta_ref, group):
    packed = columns_ref[group, rows, :]
    wide = packed.astype(jnp.float32)
    for k in range(GRID):
        scaled = wide if k == 0 else wide * scale_ref[k, pl.ds(group, 1), :]
        top = jnp.max(jnp.abs(scaled), axis=1, keepdims=True) + 1e-06
        v = scaled * (7.0 / top)
        r = v - jnp.round(v)
        square = r * r
        poly = jnp.full_like(square, SINE[-1])
        for coefficient in SINE[-2::-1]:
            poly = poly * square + coefficient
        shift = (r * poly) * top
        if k:
            shift = shift * inverse_ref[k, pl.ds(group, 1), :]
        dequant = (wide - shift).astype(jnp.bfloat16)
        lanes = group * GROUP if isinstance(group, int) else pl.multiple_of(group * GROUP, GROUP)
        delta_ref[k * UNIT : (k + 1) * UNIT, pl.ds(lanes, GROUP)] = dequant - packed


def quantize_kernel(lead):
    def body(columns_ref, scale_ref, inverse_ref, deltas):
        @pl.loop(0, deltas.shape[0])
        def _(unit):
            rows = pl.ds(pl.multiple_of(lead + unit * UNIT, 32), UNIT)

            @pl.loop(0, GROUPS, step=4)
            def _(group):
                for at in range(4):
                    quantize(columns_ref, rows, scale_ref, inverse_ref, deltas.at[unit], group + at)

    return body


def multiply(delta, tokens, out_refs, unit):
    out = lax.dot_general(
        delta[...], tokens[...], (((1,), (1,)), ((), ())), preferred_element_type=jnp.float32
    ).astype(jnp.bfloat16)
    for k in range(GRID):
        for hops in range(NX):
            at = k * UNIT + hops * ROWS
            out_refs[hops][unit, k] = out[at : at + ROWS, :]


def first_kernel():
    def body(*refs):
        core_ref, deltas, own, other = refs[0], refs[1:3], refs[3:7], refs[7:11]
        out_refs, kept, tokens, done = refs[11:15], *refs[15:]
        at_own = pl.multiple_of(core_ref[0] * HALF, HALF)
        at_other = pl.multiple_of((1 - core_ref[0]) * HALF, HALF)
        count = TOKENS // NY
        for at in range(NY):
            tokens[at * count : (at + 1) * count, pl.ds(at_own, HALF)] = own[at][...]
            tokens[at * count : (at + 1) * count, pl.ds(at_other, HALF)] = other[at][...]
        keep = pltpu.make_async_copy(tokens, kept, done)
        keep.start()
        unit = 0
        for delta in deltas:
            for at in range(delta.shape[0]):
                multiply(delta.at[at], tokens, out_refs, unit)
                unit += 1
        keep.wait()

    return body


def piece_kernel(first, units):
    def body(columns_ref, scale_ref, inverse_ref, kept, *refs):
        out_refs, (tokens, done), deltas = refs[:NX], refs[NX : NX + 2], refs[NX + 2 :]
        fetch = pltpu.make_async_copy(kept, tokens, done)
        fetch.start()
        for unit in range(units):
            delta = deltas[unit % 2]
            rows = slice((first + unit) * UNIT, (first + unit + 1) * UNIT)
            for group in range(GROUPS):
                quantize(columns_ref, rows, scale_ref, inverse_ref, delta, group)
            if unit == 0:
                fetch.wait()
            multiply(delta, tokens, out_refs, unit)

    return body


def error_kernel(*refs):
    *parts, sums_ref, total_ref = refs
    rows = []
    for k in range(GRID):
        for piece in range(len(PIECES)):
            shares = parts[piece * NX : (piece + 1) * NX]
            for unit in range(shares[0].shape[0]):
                block = shares[0][unit, k].astype(jnp.float32)
                for share in shares[1:]:
                    block += share[unit, k].astype(jnp.float32)
                block = block * block
                lanes = block[:, :128]
                for at in range(128, TOKENS, 128):
                    lanes += block[:, at : at + 128]
                rows.append(lanes)
    sums = jnp.sum(jnp.concatenate(rows, axis=0).T, axis=0, keepdims=True)
    width = UNITS * ROWS
    for k in range(GRID):
        row = sums[:, k * width : (k + 1) * width]
        sums_ref[k : k + 1, :] = row
        total_ref[:, k : k + 1] = jnp.sum(row, axis=1, keepdims=True)


def kernel(body, out_shape, limit=14, flops=0, **more):
    params = pltpu.CompilerParams(vmem_limit_bytes=limit * MIB)
    if flops:
        more["cost_estimate"] = pl.CostEstimate(flops=flops, transcendentals=0, bytes_accessed=0)
    return pl.pallas_call(body, out_shape=out_shape, compiler_params=params, **more)


def spread(value, axes, size):
    wide = jnp.broadcast_to(value[None], (size, *value.shape))
    return lax.all_to_all(wide, axes, 0, 0, tiled=True)


def shifted(value, axis, hops):
    size = lax.axis_size(axis)
    return lax.ppermute(value, axis, [(i, (i + hops) % size) for i in range(size)])


def after(value, *others):
    return lax.optimization_barrier((value, *others))[0]


def search(activations, weight):
    array = jax.ShapeDtypeStruct
    f32, bf16 = jnp.float32, jnp.bfloat16
    smem, local = pl.BlockSpec(memory_space=pltpu.SMEM), pl.BlockSpec(memory_space=pltpu.VMEM)
    core = lax.axis_index("dp_2").reshape(1)
    packed = kernel(pack_tokens, array((NC * OWN, HALF), bf16))(activations)
    turn = [(x * NY + y, y * NY + x) for x in range(NX) for y in range(NY)]
    turned = lax.ppermute(packed, ("dp_0", "tensor"), turn)
    columns = kernel(
        split_columns, [array((NZ * NC, u * UNIT, GROUP), bf16) for u in SENDS], in_specs=[smem, local]
    )(lax.axis_index("dp_0").reshape(1), weight)
    merged = array((NZ * NC, LEAD + SENDS[0] * UNIT, GROUP), bf16)
    merged = kernel(merge_kernel, merged)(turned, columns[0])
    received = [lax.all_to_all(merged, ZC, 0, 0, tiled=True)]
    half = array((HALF // GROUP, GROUP), f32)
    joined, sums = kernel(join_tokens, [array((TOKENS // NY, HALF), bf16), half])(received[0])
    for at in (1, 2):
        part = after(columns[at], joined, received[-1])
        received.append(lax.all_to_all(part, ZC, 0, 0, tiled=True))

    around = [shifted(sums, "tensor", hops) for hops in (2, 1, 3)]
    sums = (sums + around[0]) + (around[1] + around[2])
    mean = kernel(
        mean_kernel, array((GROUPS, GROUP), f32), in_specs=[smem, local, local]
    )(core, sums, shifted(sums, "dp_2", 1))
    around = [shifted(mean, "dp_0", hops) for hops in (2, 1, 3)]
    scale, inverse = kernel(scale_kernel, [array((GRID, GROUPS, GROUP), f32)] * 2)(mean, *around)

    parts = [joined] + [shifted(joined, "tensor", hops) for hops in (2, 1, 3)]
    parts += [shifted(part, "dp_2", 1) for part in parts]

    far = pl.BlockSpec(memory_space=pltpu.HBM)
    gathered = [pltpu.VMEM((TOKENS, BLOCK), bf16), pltpu.SemaphoreType.DMA]
    shares = []
    for at, (source, first, units) in enumerate(PIECES):
        out_shape = [array((units, GRID, ROWS, TOKENS), bf16)] * NX
        work = units * GRID * UNIT * TOKENS * BLOCK
        if at == 0:
            deltas = []
            for send, lead in ((0, LEAD), (1, 0)):
                quantized = array((SENDS[send], GRID * UNIT, BLOCK), bf16)
                step = kernel(quantize_kernel(lead), quantized, flops=2 * work)
                deltas.append(step(received[send], scale, inverse))
            *partial, tokens = kernel(
                first_kernel(), out_shape + [pltpu.HBM((TOKENS, BLOCK), bf16)], flops=work,
                in_specs=[smem] + [local] * 10,
                out_specs=[local] * NX + [far],
                scratch_shapes=gathered,
            )(core, *deltas, *parts)
        else:
            partial = kernel(
                piece_kernel(first, units),
                out_shape,
                flops=3 * work,
                in_specs=[local] * 3 + [far],
                scratch_shapes=gathered + [pltpu.VMEM((GRID * UNIT, BLOCK), bf16)] * min(units, 2),
            )(after(received[source], shares[-NX]), scale, inverse, pltpu.with_memory_space_constraint(tokens, pltpu.HBM))
        shares += [partial[0]] + [shifted(partial[hops], "dp_0", hops) for hops in (2, 1, 3)]
    sums, totals = kernel(error_kernel, [array((GRID, UNITS * ROWS), f32), array((1, GRID), f32)])(*shares)
    totals = totals + shifted(totals, "dp_2", 1)
    around = [shifted(totals, "dp_0", hops) for hops in (2, 1, 3)]
    totals = (totals + around[0]) + (around[1] + around[2])
    own_mean = lax.dynamic_slice_in_dim(after(mean, sums).reshape(-1), lax.axis_index(ZC) * GROUP, GROUP)
    errors = jnp.sum(spread(totals, ("dp_1", "tensor"), NZ * NY), axis=0).reshape(GRID) / (TOKENS * F)
    column_errors = after(sums, totals) / TOKENS
    return (own_mean, column_errors, errors)


def solution(mesh):
    torus = Mesh(
        mesh.devices.reshape(NX, NZ, NC, mesh.shape["tensor"]), ("dp_0", "dp_1", "dp_2", "tensor")
    )
    placed = (P(DP, "tensor"), P(DP, "tensor"))
    return jax.shard_map(
        search,
        mesh=torus,
        in_specs=placed,
        out_specs=(P(DP), P(None, TENSOR_DP), P()),
        check_vma=False,
    )
```

```python
import jax
import jax.numpy as jnp
from jax import lax
from jax.experimental import pallas as pl
from jax.experimental.pallas import tpu as pltpu
from jax.sharding import Mesh
from jax.sharding import PartitionSpec as P

D = 8192
F = 28672
GROUP = 128
GRID = 4
TOKENS = 768
DP = ("dp_0", "dp_1", "dp_2")
TENSOR_DP = ("tensor", "dp_0", "dp_1", "dp_2")
ZC = ("dp_1", "dp_2")
NX, NZ, NC, NY = 4, 8, 2, 4
UNITS = 7
ROWS = 16
UNIT = NX * ROWS
BLOCK = D // NX
GROUPS = BLOCK // GROUP
SENDS = (1, 3, 3)
PIECES = ((None, 0, 4), (2, 0, 3))
MIB = 1 << 20
HALF = BLOCK // 2
OWN = TOKENS // (NX * NZ * NC)
LEAD = OWN * HALF // GROUP

SINE = tuple(
    c / 7.0
    for c in (
        0.9999996039230294,
        -6.579691569847717,
        12.98643599053418,
        -12.188101430391939,
        6.558041838366218,
        -1.9530314806292366,
    )
)


def starts():
    first, out = 0, []
    for units in SENDS:
        out.append(first)
        first += units
    return out


def split_columns(x_ref, weight_ref, *out_refs):
    for block in range(weight_ref.shape[1] // 128):
        turned = weight_ref[:, block * 128 : (block + 1) * 128].T
        for piece in range(128 // ROWS):
            column = block * 128 + piece * ROWS
            x, rest = divmod(column, F // NY // NX)
            owner, rest = divmod(rest, UNITS * ROWS)
            unit = rest // ROWS
            hops = (x + NX - x_ref[0]) % NX
            for out, first, units in zip(out_refs, starts(), SENDS):
                if first <= unit < first + units:
                    at = pl.multiple_of(((unit - first) * NX + hops) * ROWS, ROWS)
                    out[owner, pl.ds(at, ROWS), :] = turned[piece * ROWS : (piece + 1) * ROWS, :]


def pack_tokens(tokens_ref, out_ref):
    out_ref[:OWN, :] = tokens_ref[:, :HALF]
    out_ref[OWN:, :] = tokens_ref[:, HALF:]


def merge_kernel(tokens_ref, columns_ref, out_ref):
    for half in range(NC):
        for block in range(HALF // GROUP):
            rows = tokens_ref[half * OWN : (half + 1) * OWN, block * GROUP : (block + 1) * GROUP]
            for z in range(NZ):
                out_ref[z * NC + half, block * OWN : (block + 1) * OWN, :] = rows
    out_ref[:, LEAD:, :] = columns_ref[...]


def join_tokens(parts_ref, out_ref, sums_ref):
    for block in range(HALF // GROUP):
        lanes = slice(block * GROUP, (block + 1) * GROUP)
        total = jnp.zeros((OWN, GROUP), jnp.float32)
        for at in range(NZ * NC):
            rows = parts_ref[at, block * OWN : (block + 1) * OWN, :]
            out_ref[at * OWN : (at + 1) * OWN, lanes] = rows
            total += jnp.abs(rows.astype(jnp.float32))
        sums_ref[block : block + 1, :] = jnp.sum(total, axis=0, keepdims=True)


def mean_kernel(core_ref, own_ref, other_ref, mean_ref):
    rows = HALF // GROUP
    own = pl.multiple_of(core_ref[0] * rows, rows)
    other = pl.multiple_of((1 - core_ref[0]) * rows, rows)
    mean_ref[pl.ds(own, rows), :] = own_ref[...] / TOKENS + 1e-06
    mean_ref[pl.ds(other, rows), :] = other_ref[...] / TOKENS + 1e-06


def scale_kernel(mean_0, mean_1, mean_2, mean_3, scale_ref, inverse_ref):
    logs = [jnp.log(mean[...]) for mean in (mean_0, mean_1, mean_2, mean_3)]
    for k in range(GRID):
        raws = [jnp.exp((k / GRID) * log) for log in logs]
        top = jnp.max(jnp.maximum(jnp.maximum(raws[0], raws[1]), jnp.maximum(raws[2], raws[3])))
        bottom = jnp.min(jnp.minimum(jnp.minimum(raws[0], raws[1]), jnp.minimum(raws[2], raws[3])))
        scale = raws[0] / jnp.sqrt(top * bottom)
        scale_ref[k] = scale
        inverse_ref[k] = 1.0 / scale


def quantize(columns_ref, rows, scale_ref, inverse_ref, delta_ref, group):
    packed = columns_ref[group, rows, :]
    wide = packed.astype(jnp.float32)
    for k in range(GRID):
        scaled = wide if k == 0 else wide * scale_ref[k, pl.ds(group, 1), :]
        top = jnp.max(jnp.abs(scaled), axis=1, keepdims=True) + 1e-06
        v = scaled * (7.0 / top)
        r = v - jnp.round(v)
        square = r * r
        poly = jnp.full_like(square, SINE[-1])
        for coefficient in SINE[-2::-1]:
            poly = poly * square + coefficient
        shift = (r * poly) * top
        if k:
            shift = shift * inverse_ref[k, pl.ds(group, 1), :]
        dequant = (wide - shift).astype(jnp.bfloat16)
        lanes = group * GROUP if isinstance(group, int) else pl.multiple_of(group * GROUP, GROUP)
        delta_ref[k * UNIT : (k + 1) * UNIT, pl.ds(lanes, GROUP)] = dequant - packed


def quantize_kernel(lead):
    def body(columns_ref, scale_ref, inverse_ref, deltas):
        @pl.loop(0, deltas.shape[0])
        def _(unit):
            rows = pl.ds(pl.multiple_of(lead + unit * UNIT, 32), UNIT)

            @pl.loop(0, GROUPS, step=4)
            def _(group):
                for at in range(4):
                    quantize(columns_ref, rows, scale_ref, inverse_ref, deltas.at[unit], group + at)

    return body


def multiply(delta, tokens, out_refs, unit):
    out = lax.dot_general(
        tokens[...], delta[...], (((1,), (1,)), ((), ())), preferred_element_type=jnp.float32
    )
    out = out.T.astype(jnp.bfloat16)
    for k in range(GRID):
        for hops in range(NX):
            at = k * UNIT + hops * ROWS
            out_refs[hops][unit, k] = out[at : at + ROWS, :]


def first_kernel():
    def body(*refs):
        core_ref, deltas, own, other = refs[0], refs[1:3], refs[3:7], refs[7:11]
        out_refs, kept, tokens, done = refs[11:15], *refs[15:]
        at_own = pl.multiple_of(core_ref[0] * HALF, HALF)
        at_other = pl.multiple_of((1 - core_ref[0]) * HALF, HALF)
        count = TOKENS // NY
        for at in range(NY):
            tokens[at * count : (at + 1) * count, pl.ds(at_own, HALF)] = own[at][...]
            tokens[at * count : (at + 1) * count, pl.ds(at_other, HALF)] = other[at][...]
        keep = pltpu.make_async_copy(tokens, kept, done)
        keep.start()
        unit = 0
        for delta in deltas:
            for at in range(delta.shape[0]):
                multiply(delta.at[at], tokens, out_refs, unit)
                unit += 1
        keep.wait()

    return body


def piece_kernel(first, units):
    def body(columns_ref, scale_ref, inverse_ref, kept, *refs):
        out_refs, (tokens, done), deltas = refs[:NX], refs[NX : NX + 2], refs[NX + 2 :]
        fetch = pltpu.make_async_copy(kept, tokens, done)
        fetch.start()
        for unit in range(units):
            delta = deltas[unit % 2]
            rows = slice((first + unit) * UNIT, (first + unit + 1) * UNIT)
            for group in range(GROUPS):
                quantize(columns_ref, rows, scale_ref, inverse_ref, delta, group)
            if unit == 0:
                fetch.wait()
            multiply(delta, tokens, out_refs, unit)

    return body


def error_kernel(*refs):
    *parts, sums_ref, total_ref = refs
    rows = []
    for k in range(GRID):
        for piece in range(len(PIECES)):
            shares = parts[piece * NX : (piece + 1) * NX]
            for unit in range(shares[0].shape[0]):
                block = shares[0][unit, k].astype(jnp.float32)
                for share in shares[1:]:
                    block += share[unit, k].astype(jnp.float32)
                block = block * block
                lanes = block[:, :128]
                for at in range(128, TOKENS, 128):
                    lanes += block[:, at : at + 128]
                rows.append(lanes)
    sums = jnp.sum(jnp.concatenate(rows, axis=0).T, axis=0, keepdims=True)
    width = UNITS * ROWS
    for k in range(GRID):
        row = sums[:, k * width : (k + 1) * width]
        sums_ref[k : k + 1, :] = row
        total_ref[:, k : k + 1] = jnp.sum(row, axis=1, keepdims=True)


def kernel(body, out_shape, limit=14, flops=0, **more):
    params = pltpu.CompilerParams(vmem_limit_bytes=limit * MIB)
    if flops:
        more["cost_estimate"] = pl.CostEstimate(flops=flops, transcendentals=0, bytes_accessed=0)
    return pl.pallas_call(body, out_shape=out_shape, compiler_params=params, **more)


def spread(value, axes, size):
    wide = jnp.broadcast_to(value[None], (size, *value.shape))
    return lax.all_to_all(wide, axes, 0, 0, tiled=True)


def shifted(value, axis, hops):
    size = lax.axis_size(axis)
    return lax.ppermute(value, axis, [(i, (i + hops) % size) for i in range(size)])


def after(value, *others):
    return lax.optimization_barrier((value, *others))[0]


def search(activations, weight):
    array = jax.ShapeDtypeStruct
    f32, bf16 = jnp.float32, jnp.bfloat16
    smem, local = pl.BlockSpec(memory_space=pltpu.SMEM), pl.BlockSpec(memory_space=pltpu.VMEM)
    core = lax.axis_index("dp_2").reshape(1)
    packed = kernel(pack_tokens, array((NC * OWN, HALF), bf16))(activations)
    turn = [(x * NY + y, y * NY + x) for x in range(NX) for y in range(NY)]
    turned = lax.ppermute(packed, ("dp_0", "tensor"), turn)
    columns = kernel(
        split_columns, [array((NZ * NC, u * UNIT, GROUP), bf16) for u in SENDS], in_specs=[smem, local]
    )(lax.axis_index("dp_0").reshape(1), weight)
    merged = array((NZ * NC, LEAD + SENDS[0] * UNIT, GROUP), bf16)
    merged = kernel(merge_kernel, merged)(turned, columns[0])
    received = [lax.all_to_all(merged, ZC, 0, 0, tiled=True)]
    half = array((HALF // GROUP, GROUP), f32)
    joined, sums = kernel(join_tokens, [array((TOKENS // NY, HALF), bf16), half])(received[0])
    for at in (1, 2):
        part = after(columns[at], joined, received[-1])
        received.append(lax.all_to_all(part, ZC, 0, 0, tiled=True))

    around = [shifted(sums, "tensor", hops) for hops in (2, 1, 3)]
    sums = (sums + around[0]) + (around[1] + around[2])
    mean = kernel(
        mean_kernel, array((GROUPS, GROUP), f32), in_specs=[smem, local, local]
    )(core, sums, shifted(sums, "dp_2", 1))
    around = [shifted(mean, "dp_0", hops) for hops in (2, 1, 3)]
    scale, inverse = kernel(scale_kernel, [array((GRID, GROUPS, GROUP), f32)] * 2)(mean, *around)

    parts = [joined] + [shifted(joined, "tensor", hops) for hops in (2, 1, 3)]
    parts += [shifted(part, "dp_2", 1) for part in parts]

    far = pl.BlockSpec(memory_space=pltpu.HBM)
    gathered = [pltpu.VMEM((TOKENS, BLOCK), bf16), pltpu.SemaphoreType.DMA]
    shares = []
    for at, (source, first, units) in enumerate(PIECES):
        out_shape = [array((units, GRID, ROWS, TOKENS), bf16)] * NX
        work = units * GRID * UNIT * TOKENS * BLOCK
        if at == 0:
            deltas = []
            for send, lead in ((0, LEAD), (1, 0)):
                quantized = array((SENDS[send], GRID * UNIT, BLOCK), bf16)
                step = kernel(quantize_kernel(lead), quantized, flops=2 * work)
                deltas.append(step(received[send], scale, inverse))
            *partial, tokens = kernel(
                first_kernel(), out_shape + [pltpu.HBM((TOKENS, BLOCK), bf16)], flops=work,
                in_specs=[smem] + [local] * 10,
                out_specs=[local] * NX + [far],
                scratch_shapes=gathered,
            )(core, *deltas, *parts)
        else:
            partial = kernel(
                piece_kernel(first, units),
                out_shape,
                flops=3 * work,
                in_specs=[local] * 3 + [far],
                scratch_shapes=gathered + [pltpu.VMEM((GRID * UNIT, BLOCK), bf16)] * min(units, 2),
            )(after(received[source], shares[-NX]), scale, inverse, pltpu.with_memory_space_constraint(tokens, pltpu.HBM))
        shares += [partial[0]] + [shifted(partial[hops], "dp_0", hops) for hops in (2, 1, 3)]
    sums, totals = kernel(error_kernel, [array((GRID, UNITS * ROWS), f32), array((1, GRID), f32)])(*shares)
    own_mean = lax.dynamic_slice_in_dim(after(mean, sums).reshape(-1), lax.axis_index(ZC) * GROUP, GROUP)
    errors = jnp.sum(spread(totals, ("dp_0", "dp_1", "dp_2", "tensor"), NX * NZ * NC * NY), axis=0).reshape(GRID) / (TOKENS * F)
    column_errors = sums / TOKENS
    return (own_mean, column_errors, errors)


def solution(mesh):
    torus = Mesh(
        mesh.devices.reshape(NX, NZ, NC, mesh.shape["tensor"]), ("dp_0", "dp_1", "dp_2", "tensor")
    )
    placed = (P(DP, "tensor"), P(DP, "tensor"))
    return jax.shard_map(
        search,
        mesh=torus,
        in_specs=placed,
        out_specs=(P(DP), P(None, TENSOR_DP), P()),
        check_vma=False,
    )
```
